256 devices in a mesh: grp: 2 (over x_hi), seq: 64 (over z, y, core), mp: 2 (over x_lo).
Axes of the slice: x: 4 (x_hi: 2, x_lo: 2; x = x_hi * 2 + x_lo), y: 4, z: 8, core: 2. Of those that a mesh axis runs over, the one named last changes fastest.
Arguments:
- frames: bfloat16 [12288, 8192], P(('grp', 'seq'), 'mp'), may hold values from -80 to 80
- token_session: int32 [12288], P(('grp', 'seq')), may hold values from 0 to 1023, as said below
- ln_gain: float32 [8192], P('mp'), may hold values from 0.3 to 1.7
- w_key: bfloat16 [8192, 512], P('mp'), may hold values from -0.0625 to 0.0625
- w_value: bfloat16 [8192, 512], P('mp'), may hold values from -0.0625 to 0.0625
- k_bias: float32 [512], P('mp'), may hold values from -4 to 4
- v_bias: float32 [512], P('mp'), may hold values from -4 to 4
- queries: bfloat16 [1024, 4096], P(('grp', 'seq'), 'mp'), may hold values from -4 to 4
- cache_key: bfloat16 [1024, 128, 512], P(('grp', 'seq'), None, 'mp'), may hold values from -11 to 11
- cache_value: bfloat16 [1024, 128, 512], P(('grp', 'seq'), None, 'mp'), may hold values from -6 to 6
- cache_start: int32 [1024], P(('grp', 'seq')), may hold values from 0 to 127
- cache_len: int32 [1024], P(('grp', 'seq')), may hold values from 1 to 128
Outputs:
- attended: bfloat16 [1024, 4096], P(('grp', 'seq'), 'mp')
The draws below stay inside these ranges and needn't reach their ends.
Inputs may be any that keep to these rules, and one draw needn't show every extreme that they name: `token_session`: each new frame token names a session; within the rows of one device at most 2 rows name sessions of one block of 8 consecutive sessions, and in every draw one such block gets exactly 2 rows from every device.
All inputs are finite; a program needn't handle non-finite values.
Results may differ from the reference program's by a relative error of at most 0.0023.
The reference program's roundings to bfloat16 on the way count: a program that leaves them out, or rounds other values in their place, can miss the bound.
Values may be sent and summed in bfloat16 or wider, within the bound.
A program may use at most 64 MiB of HBM per device.

```python
import jax
import jax.numpy as jnp
from jax import lax

D = 8192
HEAD = 128
GROUP = 8
KV_HEADS = 4
ENC_DEV = 96
STR_DEV = 8
WIN = 128
CAP = 2
ROWS = 12288
STREAMS = 1024
QH = 32


def draw_frames(key, part):
    key_rows, key_cols, key_base = jax.random.split(jax.random.fold_in(key, 3), 3)
    row_scale = jnp.exp(jax.random.uniform(key_rows, (ROWS, 1), jnp.float32) * jnp.log(10.0))
    col_scale = jnp.exp(jax.random.uniform(key_cols, (1, D), jnp.float32) * jnp.log(10.0))
    base = jnp.clip(jax.random.normal(key_base, (ROWS, D), jnp.float32), -4.0, 4.0)
    return (0.2 * base * row_scale * col_scale).astype(jnp.bfloat16)


def draw_token_session(key, part):
    blocks = ROWS // ENC_DEV
    partition_count = STREAMS // STR_DEV
    count_of_slots = partition_count * CAP
    busiest_prng_key, credit_prng_key, perturb_prng_key, selection_prng_key, displacement_prng_key = jax.random.split(jax.random.fold_in(key, 11), 5)
    busiest_slot = jax.random.randint(busiest_prng_key, (), 0, partition_count)
    extra_credit = jax.random.randint(credit_prng_key, (partition_count,), 0, 3) * 1024
    extra_credit = jnp.where(jnp.arange(partition_count, dtype=jnp.int32) == busiest_slot, 8192, extra_credit)
    slot_partition = jnp.arange(count_of_slots, dtype=jnp.int32) // CAP
    random_perturbation = jax.random.randint(perturb_prng_key, (blocks, count_of_slots), 0, 1024)
    slot_score_values = (extra_credit[slot_partition][None, :] + random_perturbation) * count_of_slots + jnp.arange(count_of_slots, dtype=jnp.int32)[None, :]
    unused, picked = lax.top_k(slot_score_values, ENC_DEV)
    target = picked // CAP
    choose = jax.random.randint(selection_prng_key, (blocks, ENC_DEV), 0, 2 * STR_DEV)
    local = jnp.where(choose < STR_DEV, choose, (choose - STR_DEV) // 2)
    offsets = jax.random.randint(displacement_prng_key, (partition_count,), 0, STR_DEV)
    local = jnp.mod(local + offsets[target], STR_DEV)
    return (target * STR_DEV + local).reshape(ROWS).astype(jnp.int32)


def draw_queries(key, part):
    key_base = jax.random.fold_in(key, 13)
    base = jnp.clip(jax.random.normal(key_base, (STREAMS, KV_HEADS, GROUP, HEAD), jnp.float32), -4.0, 4.0)
    return base.reshape(STREAMS, KV_HEADS * GROUP * HEAD).astype(jnp.bfloat16)


def draw_cache_key(key, part):
    key_base = jax.random.fold_in(jax.random.fold_in(key, 17), 0)
    base = jnp.clip(jax.random.normal(key_base, (STREAMS, WIN, KV_HEADS, HEAD), jnp.float32), -4.0, 4.0)
    return base.reshape(STREAMS, WIN, KV_HEADS * HEAD).astype(jnp.bfloat16)


def plant(drawn, key, least, high):
    spot = [jax.random.randint(jax.random.fold_in(key, axis), (), 0, length) for axis, length in enumerate(drawn.shape)]
    widest = drawn.shape.index(max(drawn.shape))
    beside = spot[:widest] + [(spot[widest] + 1) % drawn.shape[widest]] + spot[widest + 1:]
    return drawn.at[tuple(spot)].set(least).at[tuple(beside)].set(high)


def block_levels(rng, shape, pieces, low, high):
    gain, own = 1.0, jax.random.fold_in(rng, 6)
    for axis_at, blocks in pieces:
        heights = jnp.exp(jax.random.uniform(jax.random.fold_in(own, axis_at), (blocks,), jnp.float32, low / len(pieces), high / len(pieces)))
        gain = gain * jnp.repeat(heights, shape[axis_at] // blocks).reshape([-1 if axis == axis_at else 1 for axis in range(len(shape))])
    return gain


def centred(key, dims, scale, bound, cuts=(), kind=jnp.bfloat16):
    entries = scale * jax.random.normal(key, dims, jnp.float32)
    if cuts:
        entries = entries * block_levels(key, dims, cuts, -0.22, 0.18)
    return jnp.clip(entries, -bound, bound).astype(kind)


def setup_inputs(seed: int = 0) -> dict:
    arg_keys = jax.random.split(jax.random.key(seed), 13)
    frames = draw_frames(jax.random.fold_in(arg_keys[12], 71), 0)
    token_session = draw_token_session(jax.random.fold_in(arg_keys[12], 71), 0)
    ln_gain = jnp.clip(0.3 + 1.40000004 * jax.random.uniform(arg_keys[2], (D,), jnp.float32) ** block_levels(arg_keys[2], (D,), ((0, 2),), -0.2, 0.2), 0.3, 1.7)
    w_key = centred(arg_keys[3], (D, KV_HEADS * HEAD), D ** -0.5, 0.0625, ((0, 2),))
    w_value = centred(arg_keys[4], (D, KV_HEADS * HEAD), D ** -0.5, 0.0625, ((0, 2),))
    k_bias = centred(arg_keys[5], (KV_HEADS * HEAD,), 1.0, 4.0, ((0, 2),), jnp.float32)
    v_bias = centred(arg_keys[6], (KV_HEADS * HEAD,), 1.0, 4.0, ((0, 2),), jnp.float32)
    queries = draw_queries(jax.random.fold_in(arg_keys[12], 71), 0)
    cache_key = draw_cache_key(jax.random.fold_in(arg_keys[12], 71), 0)
    cache_value = centred(arg_keys[9], (STREAMS, WIN, KV_HEADS * HEAD), 1.0, 6.0, ((0, 128), (2, 2)))
    cache_start = plant(jax.random.randint(arg_keys[10], (STREAMS,), 0, WIN), jax.random.fold_in(arg_keys[10], 1), 0, WIN - 1).astype(jnp.int32)
    cache_len = plant(jax.random.randint(arg_keys[11], (STREAMS,), 1, WIN + 1), jax.random.fold_in(arg_keys[11], 1), 1, WIN).astype(jnp.int32)
    return dict(frames=frames, token_session=token_session, ln_gain=ln_gain, w_key=w_key, w_value=w_value, k_bias=k_bias, v_bias=v_bias, queries=queries, cache_key=cache_key, cache_value=cache_value, cache_start=cache_start, cache_len=cache_len)


epsilon = 1e-06

def project_block(frame_rows, ln_gain, w_key, w_value, k_bias, v_bias):
    values32 = frame_rows.astype(jnp.float32)
    inverse_rms = lax.rsqrt(lax.optimization_barrier(jnp.mean(values32 * values32, axis=1)) + epsilon)
    normed = (values32 * inverse_rms[:, None] * ln_gain[None, :]).astype(jnp.bfloat16)
    new_keys = jnp.dot(normed, w_key, preferred_element_type=jnp.float32) + k_bias[None, :]
    new_values = jnp.dot(normed, w_value, preferred_element_type=jnp.float32) + v_bias[None, :]
    return (new_keys.astype(jnp.bfloat16), new_values.astype(jnp.bfloat16))

def reference(frames, token_session, ln_gain, w_key, w_value, k_bias, v_bias, queries, cache_key, cache_value, cache_start, cache_len):
    blocks = frames.reshape(ROWS // ENC_DEV, ENC_DEV, D)

    def one_block(frame_block):
        return project_block(frame_block, ln_gain, w_key, w_value, k_bias, v_bias)
    new_keys, new_values = lax.map(one_block, blocks)
    new_keys = new_keys.reshape(ROWS, KV_HEADS, HEAD).astype(jnp.float32)
    new_values = new_values.reshape(ROWS, KV_HEADS, HEAD).astype(jnp.float32)
    score_scale = HEAD ** (-0.5)
    query_heads = queries.astype(jnp.float32).reshape(STREAMS, KV_HEADS, GROUP, HEAD)
    cached_keys = cache_key.astype(jnp.float32).reshape(STREAMS, WIN, KV_HEADS, HEAD)
    cached_values = cache_value.astype(jnp.float32).reshape(STREAMS, WIN, KV_HEADS, HEAD)
    cached_scores = jnp.einsum('sghd,swgd->sghw', query_heads, cached_keys) * score_scale
    positions = jnp.arange(WIN, dtype=jnp.int32)
    live_slots = jnp.mod(positions[None, :] - cache_start[:, None], WIN) < cache_len[:, None]
    cached_scores = jnp.where(live_slots[:, None, None, :], cached_scores, -jnp.inf)
    row_queries = query_heads[token_session]
    fresh_scores = jnp.einsum('rghd,rgd->rgh', row_queries, new_keys) * score_scale
    fresh_largest = jax.ops.segment_max(fresh_scores, token_session, num_segments=STREAMS)
    largest = jnp.maximum(lax.optimization_barrier(jnp.max(cached_scores, axis=3)), fresh_largest)
    cached_exp = jnp.exp(cached_scores - largest[..., None])
    fresh_exp = jnp.exp(fresh_scores - largest[token_session])
    totals = lax.optimization_barrier(jnp.sum(cached_exp, axis=3)) + jax.ops.segment_sum(fresh_exp, token_session, num_segments=STREAMS)
    cached_weights = (cached_exp / totals[..., None]).astype(jnp.bfloat16)
    fresh_weights = (fresh_exp / totals[token_session]).astype(jnp.bfloat16)
    attended = jnp.einsum('sghw,swgd->sghd', cached_weights.astype(jnp.float32), cached_values)
    fresh_terms = fresh_weights.astype(jnp.float32)[..., None] * new_values[:, :, None, :]
    attended = attended + jax.ops.segment_sum(fresh_terms, token_session, num_segments=STREAMS)
    return attended.reshape(STREAMS, QH * HEAD).astype(jnp.bfloat16)
```

```python
import functools

import jax
import jax.numpy as jnp
from jax import lax
from jax.experimental import pallas as pl
from jax.experimental.pallas import tpu as pltpu
from jax.sharding import PartitionSpec as P

HEAD = 128
GROUP = 8
EPSILON = 1e-6
MESH = pl.DeviceIdType.MESH

NZ, NY, NC, NG = 8, 4, 2, 2
PARTS = NG * NZ * NY * NC
F32 = jnp.float32
BF16 = jnp.bfloat16


def kernel(
    tok_hbm, frames_hbm, gain_hbm, wk_hbm, wv_hbm, kb_hbm, vb_hbm, q_hbm, ck_hbm, cv_hbm, start_hbm, len_hbm,
    out_ref,
    tok, frames, gain, weights, kb, vb, q, ck, cv, start, length,
    normed, square_out, square_in, part_out, part_in, own_part, onehot, send, recv, send_id, recv_id, cached,
    sem_in, sem_w, sem_sq, sem_part_s, sem_part_r, sem_data, sem_id, know1, know2, know3,
):
    g, s, m = lax.axis_index("grp"), lax.axis_index("seq"), lax.axis_index("mp")
    core, y, z = lax.rem(s, NC), lax.rem(s // NC, NY), s // (NC * NY)
    me = g * (NZ * NY * NC) + s
    rows, depth = frames.shape
    half = kb.shape[1]

    def seq_of(zz, yy, cc):
        return zz * (NY * NC) + yy * NC + cc

    def turned(dg, dz, dy, dc):
        return (
            lax.rem(g + dg, NG),
            seq_of(lax.rem(z + dz, NZ), lax.rem(y + dy, NY), lax.rem(core + dc, NC)),
            m,
        )

    other = (g, s, 1 - m)

    def tell(sem, devices):
        for device in devices:
            pl.semaphore_signal(sem, inc=1, device_id=device, device_id_type=MESH)

    barrier = pltpu.get_barrier_semaphore()
    far_core = seq_of(z, y, 1 - core)
    near = [
        other, (1 - g, s, 1 - m), (g, far_core, 1 - m), (1 - g, far_core, 1 - m), (g, far_core, m),
        turned(0, 1, 0, 0), turned(0, NZ - 1, 0, 0), turned(0, 0, 1, 0), turned(0, 0, NY - 1, 0),
    ]
    tell(barrier, near)

    chunk = 32
    loads = [
        pltpu.make_async_copy(
            frames_hbm.at[pl.ds(i * chunk, chunk)], frames.at[pl.ds(i * chunk, chunk)], sem_in.at[i]
        )
        for i in range(rows // chunk)
    ]
    n = len(loads)
    gain_load = pltpu.make_async_copy(gain_hbm, gain, sem_in.at[n])
    tok_load = pltpu.make_async_copy(tok_hbm, tok, sem_in.at[n + 1])
    small = [
        pltpu.make_async_copy(kb_hbm, kb, sem_in.at[n + 2]),
        pltpu.make_async_copy(vb_hbm, vb, sem_in.at[n + 3]),
    ]
    late = [
        pltpu.make_async_copy(q_hbm, q, sem_in.at[n + 4]),
        pltpu.make_async_copy(ck_hbm, ck, sem_in.at[n + 5]),
        pltpu.make_async_copy(cv_hbm, cv, sem_in.at[n + 6]),
        pltpu.make_async_copy(start_hbm, start, sem_in.at[n + 7]),
        pltpu.make_async_copy(len_hbm, length, sem_in.at[n + 8]),
    ]
    for load in loads:
        load.start()
    gain_load.start()
    tok_load.start()
    weight_loads = []
    for i, (source, side) in enumerate(((wk_hbm, 1 - m), (wv_hbm, 1 - m), (wk_hbm, m), (wv_hbm, m))):
        load = pltpu.make_async_copy(
            source.at[:, pl.ds(pl.multiple_of(side * half, half), half)], weights.at[i], sem_w.at[i]
        )
        load.start()
        weight_loads.append(load)
    for load in small + late:
        load.start()

    lanes = 128
    square_out[...] = jnp.zeros_like(square_out)
    sums = []
    for i, load in enumerate(loads):
        load.wait()
        total = jnp.zeros((chunk, lanes), F32)
        for j in range(depth // lanes):
            x = frames[pl.ds(i * chunk, chunk), pl.ds(j * lanes, lanes)].astype(F32)
            total = total + x * x
        sums.append(total)
    sums.append(jnp.zeros((lanes - rows, lanes), F32))
    own_squares = jnp.sum(jnp.concatenate(sums, axis=0).T, axis=0, keepdims=True)
    square_out[...] = own_squares
    pl.semaphore_wait(barrier, len(near))
    square_copy = pltpu.make_async_remote_copy(
        square_out, square_in, sem_sq.at[0], sem_sq.at[1], device_id=other, device_id_type=MESH
    )
    square_copy.start()
    tell(know1, [turned(0, 1, 0, 0), turned(0, NZ - 1, 0, 0), turned(0, 0, 1, 0), turned(0, 0, NY - 1, 0), other])

    tok_load.wait()
    row_at = lax.broadcasted_iota(jnp.int32, (1, lanes), 1)
    session = jnp.concatenate([tok[...].astype(F32), jnp.full((1, lanes - rows), -8.0 * PARTS, F32)], axis=1)
    block = jnp.floor(session * 0.125)
    within = session - block * 8.0
    block_here = jnp.broadcast_to(block, (lanes, lanes))
    lane_i = lax.broadcasted_iota(jnp.int32, (lanes, lanes), 1)
    sub_i = lax.broadcasted_iota(jnp.int32, (lanes, lanes), 0)
    before = (block_here.T == block_here) & (sub_i < lane_i)
    rank = jnp.sum(before.astype(F32), axis=0, keepdims=True)
    slot = jnp.where(row_at < rows, block * 2.0 + rank, -1.0)
    slot_here = jnp.broadcast_to(slot, (lanes, lanes))
    ids = []
    for j in range(2):
        hit = slot_here == (2 * sub_i + j).astype(F32)
        ids.append(jnp.sum(jnp.where(hit, within + 1.0, 0.0), axis=1, keepdims=True))
    id_here = jnp.where(lax.rem(lane_i // 4, 2) == 0, ids[0], ids[1])
    id_here = jnp.where(lane_i // 8 == lax.rem(me, 16), id_here, 0.0)
    send_id[...] = id_here.reshape(PARTS, 1, lanes)
    for p in range(8):
        big = lax.broadcasted_iota(jnp.int32, (lanes, lanes), 0)
        hit = jnp.broadcast_to(slot, (lanes, lanes)) == (big // 4 + p * 32).astype(F32)
        for c in range(4):
            onehot[pl.ds(p * lanes, lanes), pl.ds(c * lanes, lanes)] = jnp.where(
                hit & (lax.rem(big, 4) == c), 1.0, 0.0
            ).astype(BF16)

    pl.semaphore_wait(know1, 5)
    line = [turned(0, 0, d, 0) for d in range(1, NY)]
    tell(know2, [turned(0, 2, 0, 0), turned(0, NZ - 2, 0, 0)] + line)

    gain_load.wait()
    square_copy.wait()
    squares = square_out[...] + square_in[...]
    inverse = lax.rsqrt(squares / (2 * depth) + EPSILON)
    inverse = jnp.broadcast_to(inverse, (lanes, lanes)).T[:rows]
    for j in range(depth // lanes):
        cols = pl.ds(j * lanes, lanes)
        normed[:, cols] = (frames[:, cols].astype(F32) * inverse * gain[:, cols]).astype(BF16)

    pl.semaphore_wait(know2, 5)
    group = [
        turned(dg, 0, dy, dc) for dg in range(NG) for dy in range(NY) for dc in range(NC) if dg or dy or dc
    ]
    tell(know3, group)

    part_copies = []
    for i in range(4):
        weight_loads[i].wait()
        product = jnp.dot(normed[...], weights[i], preferred_element_type=F32)
        if i < 2:
            part_out[i] = product
            copy = pltpu.make_async_remote_copy(
                part_out.at[i], part_in.at[i], sem_part_s.at[i], sem_part_r.at[i], device_id=other, device_id_type=MESH
            )
            copy.start()
            part_copies.append(copy)
        else:
            own_part[i - 2] = product
    for load in small + late:
        load.wait()

    pl.semaphore_wait(know3, len(group))

    def peer(k):
        return turned(k // (NZ * NY * NC), lax.rem(k // (NY * NC), NZ), lax.rem(k // NC, NY), lax.rem(k, NC))

    @pl.loop(1, PARTS)
    def _(k):
        device = peer(k)
        to = device[0] * (NZ * NY * NC) + device[1]
        pltpu.make_async_remote_copy(
            send_id.at[to], recv_id.at[me], sem_id.at[0], sem_id.at[1], device_id=device, device_id_type=MESH
        ).start()

    recv_id[me] = send_id[me]

    heads = q.shape[1] // HEAD
    kv_heads = heads // GROUP
    per_shard = q.shape[0]
    stacked = jnp.concatenate([q[:, pl.ds(i * HEAD, HEAD)] for i in range(heads)], axis=0)
    scale = HEAD**-0.5
    window = ck.shape[1]
    slots = lax.broadcasted_iota(jnp.int32, (1, window), 1)
    row_session = lax.broadcasted_iota(jnp.int32, (GROUP * per_shard, lanes), 0)
    row_session = lax.rem(row_session, per_shard)
    for h in range(kv_heads):
        queries = stacked[h * GROUP * per_shard : (h + 1) * GROUP * per_shard]
        score = jnp.zeros((GROUP * per_shard, window), F32)
        for b in range(per_shard):
            keys = ck[b, :, pl.ds(h * HEAD, HEAD)]
            product = lax.dot_general(queries, keys, (((1,), (1,)), ((), ())), preferred_element_type=F32) * scale
            live = lax.rem(slots - start[b] + window, window) < length[b]
            product = jnp.where(live, product, -jnp.inf)
            score = jnp.where(row_session == b, product, score)
        cached[pl.ds(h * GROUP * per_shard, GROUP * per_shard)] = score

    parts = []
    for i, bias in enumerate((kb, vb)):
        part_copies[i].wait()
        whole = (own_part[i] + part_in[i] + bias[...]).astype(BF16)
        for h in range(kv_heads):
            parts.append(whole[:, h * HEAD : (h + 1) * HEAD])
            parts.append(jnp.zeros((lanes - rows, HEAD), BF16))
    table = jnp.concatenate(parts, axis=0)
    slotted = jnp.dot(onehot[...], table, preferred_element_type=F32).astype(BF16)
    send[...] = slotted.reshape(send.shape)

    @pl.loop(1, PARTS)
    def _(k):
        device = peer(k)
        to = device[0] * (NZ * NY * NC) + device[1]
        pltpu.make_async_remote_copy(
            send.at[to], recv.at[me], sem_data.at[0], sem_data.at[1], device_id=device, device_id_type=MESH
        ).start()

    recv[me] = send[me]

    everyone = pl.ds(0, PARTS - 1)
    pltpu.make_async_remote_copy(
        send_id.at[everyone], recv_id.at[everyone], sem_id.at[0], sem_id.at[1], device_id=other, device_id_type=MESH
    ).wait()
    lane_ids = [jnp.sum(recv_id[pl.ds(16 * i, 16)], axis=0) for i in range(8)]
    pltpu.make_async_remote_copy(
        send.at[everyone], recv.at[everyone], sem_data.at[0], sem_data.at[1], device_id=other, device_id_type=MESH
    ).wait()

    fresh_rows = recv[...].reshape(PARTS * 8, HEAD)
    fresh = lax.dot_general(stacked, fresh_rows, (((1,), (1,)), ((), ())), preferred_element_type=F32) * scale
    ids_row = jnp.concatenate(lane_ids, axis=1)
    shape = fresh.shape
    row_i = lax.broadcasted_iota(jnp.int32, shape, 0)
    col_i = lax.broadcasted_iota(jnp.int32, shape, 1)
    match = (ids_row == (lax.rem(row_i, per_shard) + 1).astype(F32)) & (
        lax.rem(col_i, 4) == row_i // (GROUP * per_shard)
    )
    fresh = jnp.where(match, fresh, -jnp.inf)
    held = cached[...]
    largest = jnp.maximum(jnp.max(held, axis=1, keepdims=True), jnp.max(fresh, axis=1, keepdims=True))
    held_exp = jnp.exp(held - largest)
    fresh_exp = jnp.exp(fresh - largest)
    total = jnp.sum(held_exp, axis=1, keepdims=True) + jnp.sum(fresh_exp, axis=1, keepdims=True)
    inverse_total = 1.0 / total
    held_weights = held_exp * inverse_total
    fresh_weights = pltpu.roll(fresh_exp * inverse_total, 2, 1).astype(BF16)
    result = jnp.dot(fresh_weights, fresh_rows, preferred_element_type=F32)
    for h in range(kv_heads):
        part = result[h * GROUP * per_shard : (h + 1) * GROUP * per_shard]
        mine = held_weights[h * GROUP * per_shard : (h + 1) * GROUP * per_shard]
        for b in range(per_shard):
            only = jnp.where(row_session == b, mine, 0.0).astype(BF16)
            part = part + jnp.dot(only, cv[b, :, pl.ds(h * HEAD, HEAD)], preferred_element_type=F32)
        for i in range(GROUP):
            out_ref[:, pl.ds((h * GROUP + i) * HEAD, HEAD)] = part[
                i * per_shard : (i + 1) * per_shard
            ].astype(BF16)


def local(
    frames, token_session, ln_gain, w_key, w_value, k_bias, v_bias, queries, cache_key, cache_value, cache_start,
    cache_len,
):
    rows, depth = frames.shape
    half = k_bias.shape[0]
    row = lambda a: a.reshape(1, -1)
    anywhere = pl.BlockSpec(memory_space=pltpu.HBM)
    dma = pltpu.SemaphoreType.DMA
    regular = pltpu.SemaphoreType.REGULAR
    vm = pltpu.VMEM
    return pl.pallas_call(
        kernel,
        out_shape=jax.ShapeDtypeStruct(queries.shape, BF16),
        in_specs=[anywhere] * 12,
        out_specs=pl.BlockSpec(memory_space=pltpu.VMEM),
        scratch_shapes=[
            vm((1, rows), jnp.int32), vm((rows, depth), BF16), vm((1, depth), F32), vm((4, depth, half), BF16),
            vm((1, half), F32), vm((1, half), F32), vm(queries.shape, BF16), vm(cache_key.shape, BF16),
            vm(cache_value.shape, BF16), pltpu.SMEM((8,), jnp.int32), pltpu.SMEM((8,), jnp.int32),
            vm((rows, depth), BF16), vm((1, 128), F32), vm((1, 128), F32), vm((2, rows, half), F32),
            vm((2, rows, half), F32), vm((2, rows, half), F32), vm((PARTS * 8, 512), BF16),
            vm((PARTS, 8, HEAD), BF16), vm((PARTS, 8, HEAD), BF16), vm((PARTS, 1, 128), F32), vm((PARTS, 1, 128), F32),
            vm((128, 128), F32),
            dma((16,)), dma((4,)), dma((2,)), dma((2,)), dma((2,)), dma((2,)), dma((2,)),
            regular, regular, regular,
        ],
        compiler_params=pltpu.CompilerParams(
            collective_id=0, has_side_effects=True, vmem_limit_bytes=67_000_000
        ),
        name="frame_attention",
    )(
        row(token_session), frames, row(ln_gain), w_key, w_value, row(k_bias), row(v_bias), queries, cache_key,
        cache_value, cache_start, cache_len,
    )


def solution(mesh):
    rows = ("grp", "seq")
    return jax.shard_map(
        local,
        mesh=mesh,
        in_specs=(
            P(rows, "mp"), P(rows), P("mp"), P("mp", None), P("mp", None), P("mp"), P("mp"), P(rows, "mp"),
            P(rows, None, "mp"), P(rows, None, "mp"), P(rows), P(rows),
        ),
        out_specs=P(rows, "mp"),
        check_vma=False,
    )
```

```python
import functools

import jax
import jax.numpy as jnp
from jax import lax
from jax.experimental import pallas as pl
from jax.experimental.pallas import tpu as pltpu
from jax.sharding import PartitionSpec as P

HEAD = 128
GROUP = 8
EPSILON = 1e-6
MESH = pl.DeviceIdType.MESH

NZ, NY, NC, NG = 8, 4, 2, 2
PARTS = NG * NZ * NY * NC
F32 = jnp.float32
BF16 = jnp.bfloat16


def kernel(
    tok_hbm, frames_hbm, gain_hbm, wk_hbm, wv_hbm, kb_hbm, vb_hbm, q_hbm, ck_hbm, cv_hbm, start_hbm, len_hbm,
    out_ref,
    tok, frames, gain, weights, kb, vb, q, ck, cv, start, length,
    normed, square_out, square_in, part_out, part_in, own_part, onehot, send, recv, line_tok, all_tok, cached,
    sem_in, sem_w, sem_sq, sem_part_s, sem_part_r, sem_data, sem_line, sem_all, know1, know2, know3,
):
    g, s, m = lax.axis_index("grp"), lax.axis_index("seq"), lax.axis_index("mp")
    core, y, z = lax.rem(s, NC), lax.rem(s // NC, NY), s // (NC * NY)
    me = g * (NZ * NY * NC) + s
    column = (g * NY + y) * NC + core
    rows, depth = frames.shape
    half = kb.shape[1]
    at_g = [g, 1 - g]
    at_z = [z] + [lax.rem(z + d, NZ) * (NY * NC) for d in range(1, NZ)]
    at_z[0] = z * (NY * NC)
    at_y = [y * NC] + [lax.rem(y + d, NY) * NC for d in range(1, NY)]
    at_core = [core, 1 - core]
    at_yc = [[at_y[dy] + at_core[dc] for dc in range(NC)] for dy in range(NY)]

    def turned(dg, dz, dy, dc):
        return (at_g[dg], at_z[dz] + at_yc[dy][dc], m)

    other = (g, s, 1 - m)

    def tell(sem, devices):
        for device in devices:
            pl.semaphore_signal(sem, inc=1, device_id=device, device_id_type=MESH)

    barrier = pltpu.get_barrier_semaphore()
    far_core = at_z[0] + at_yc[0][1]
    near = [
        other, (1 - g, s, 1 - m), (g, far_core, 1 - m), (1 - g, far_core, 1 - m), (g, far_core, m),
        turned(0, 1, 0, 0), turned(0, NZ - 1, 0, 0), turned(0, 0, 1, 0), turned(0, 0, NY - 1, 0),
    ]
    tell(barrier, near)

    chunk = 32
    loads = [
        pltpu.make_async_copy(
            frames_hbm.at[pl.ds(i * chunk, chunk)], frames.at[pl.ds(i * chunk, chunk)], sem_in.at[i]
        )
        for i in range(rows // chunk)
    ]
    n = len(loads)
    gain_load = pltpu.make_async_copy(gain_hbm, gain, sem_in.at[n])
    tok_load = pltpu.make_async_copy(tok_hbm, tok, sem_in.at[n + 1])
    small = [
        pltpu.make_async_copy(kb_hbm, kb, sem_in.at[n + 2]),
        pltpu.make_async_copy(vb_hbm, vb, sem_in.at[n + 3]),
    ]
    late = [
        pltpu.make_async_copy(q_hbm, q, sem_in.at[n + 4]),
        pltpu.make_async_copy(ck_hbm, ck, sem_in.at[n + 5]),
        pltpu.make_async_copy(cv_hbm, cv, sem_in.at[n + 6]),
        pltpu.make_async_copy(start_hbm, start, sem_in.at[n + 7]),
        pltpu.make_async_copy(len_hbm, length, sem_in.at[n + 8]),
    ]
    for load in loads:
        load.start()
    gain_load.start()
    tok_load.start()
    weight_loads = []
    for i, (source, side) in enumerate(((wk_hbm, 1 - m), (wv_hbm, 1 - m), (wk_hbm, m), (wv_hbm, m))):
        load = pltpu.make_async_copy(
            source.at[:, pl.ds(pl.multiple_of(side * half, half), half)], weights.at[i], sem_w.at[i]
        )
        load.start()
        weight_loads.append(load)
    for load in small + late:
        load.start()

    lanes = 128
    square_out[...] = jnp.zeros_like(square_out)
    sums = []
    for i, load in enumerate(loads):
        load.wait()
        total = jnp.zeros((chunk, lanes), F32)
        for j in range(depth // lanes):
            x = frames[pl.ds(i * chunk, chunk), pl.ds(j * lanes, lanes)].astype(F32)
            total = total + x * x
        sums.append(total)
    sums.append(jnp.zeros((lanes - rows, lanes), F32))
    own_squares = jnp.sum(jnp.concatenate(sums, axis=0).T, axis=0, keepdims=True)
    square_out[...] = own_squares
    pl.semaphore_wait(barrier, len(near))
    square_copy = pltpu.make_async_remote_copy(
        square_out, square_in, sem_sq.at[0], sem_sq.at[1], device_id=other, device_id_type=MESH
    )
    square_copy.start()
    tell(know1, [turned(0, 1, 0, 0), turned(0, NZ - 1, 0, 0), turned(0, 0, 1, 0), turned(0, 0, NY - 1, 0), other])

    tok_load.wait()
    padded = jnp.concatenate([tok[...].astype(F32), jnp.full((1, lanes - rows), -8.0 * PARTS, F32)], axis=1)
    line_tok[z] = padded
    row_at = lax.broadcasted_iota(jnp.int32, (1, lanes), 1)
    block = jnp.floor(padded * 0.125)
    block_here = jnp.broadcast_to(block, (lanes, lanes))
    lane_i = lax.broadcasted_iota(jnp.int32, (lanes, lanes), 1)
    sub_i = lax.broadcasted_iota(jnp.int32, (lanes, lanes), 0)
    before = (block_here.T == block_here) & (sub_i < lane_i)
    rank = jnp.sum(before.astype(F32), axis=0, keepdims=True)
    slot = jnp.where(row_at < rows, block * 2.0 + rank, -1.0)
    slot_here = jnp.broadcast_to(slot, (lanes, lanes))
    for p in range(8):
        big = lax.broadcasted_iota(jnp.int32, (lanes, lanes), 0)
        hit = jnp.broadcast_to(slot, (lanes, lanes)) == (big // 4 + p * 32).astype(F32)
        for c in range(4):
            onehot[pl.ds(p * lanes, lanes), pl.ds(c * lanes, lanes)] = jnp.where(
                hit & (lax.rem(big, 4) == c), 1.0, 0.0
            ).astype(BF16)

    pl.semaphore_wait(know1, 5)
    line = [turned(0, 0, d, 0) for d in range(1, NY)]
    tell(know2, [turned(0, 2, 0, 0), turned(0, NZ - 2, 0, 0)] + line)

    gain_load.wait()
    square_copy.wait()
    squares = square_out[...] + square_in[...]
    inverse = lax.rsqrt(squares / (2 * depth) + EPSILON)
    inverse = jnp.broadcast_to(inverse, (lanes, lanes)).T[:rows]
    for j in range(depth // lanes):
        cols = pl.ds(j * lanes, lanes)
        normed[:, cols] = (frames[:, cols].astype(F32) * inverse * gain[:, cols]).astype(BF16)

    pl.semaphore_wait(know2, 5)
    group = [
        turned(dg, 0, dy, dc) for dg in range(NG) for dy in range(NY) for dc in range(NC) if dg or dy or dc
    ]
    tell(know3, group)
    for d in range(1, NZ):
        pltpu.make_async_remote_copy(
            line_tok.at[z], line_tok.at[z], sem_line.at[0], sem_line.at[1], device_id=turned(0, d, 0, 0), device_id_type=MESH
        ).start()

    part_copies = []
    for i in range(4):
        weight_loads[i].wait()
        product = jnp.dot(normed[...], weights[i], preferred_element_type=F32)
        if i < 2:
            part_out[i] = product
            copy = pltpu.make_async_remote_copy(
                part_out.at[i], part_in.at[i], sem_part_s.at[i], sem_part_r.at[i], device_id=other, device_id_type=MESH
            )
            copy.start()
            part_copies.append(copy)
        else:
            own_part[i - 2] = product
    some = pl.ds(0, NZ - 1)
    pltpu.make_async_remote_copy(
        line_tok.at[some], line_tok.at[some], sem_line.at[0], sem_line.at[1], device_id=other, device_id_type=MESH
    ).wait()
    for device in group:
        pltpu.make_async_remote_copy(
            line_tok, all_tok.at[column], sem_all.at[0], sem_all.at[1], device_id=device, device_id_type=MESH
        ).start()
    all_tok[column] = line_tok[...]
    for load in small + late:
        load.wait()

    heads = q.shape[1] // HEAD
    kv_heads = heads // GROUP
    per_shard = q.shape[0]
    stacked = jnp.concatenate([q[:, pl.ds(i * HEAD, HEAD)] for i in range(heads)], axis=0)
    scale = HEAD**-0.5
    window = ck.shape[1]
    slots = lax.broadcasted_iota(jnp.int32, (1, window), 1)
    row_session = lax.broadcasted_iota(jnp.int32, (GROUP * per_shard, lanes), 0)
    row_session = lax.rem(row_session, per_shard)
    for h in range(kv_heads):
        queries = stacked[h * GROUP * per_shard : (h + 1) * GROUP * per_shard]
        score = jnp.zeros((GROUP * per_shard, window), F32)
        for b in range(per_shard):
            keys = ck[b, :, pl.ds(h * HEAD, HEAD)]
            product = lax.dot_general(queries, keys, (((1,), (1,)), ((), ())), preferred_element_type=F32) * scale
            live = lax.rem(slots - start[b] + window, window) < length[b]
            product = jnp.where(live, product, -jnp.inf)
            score = jnp.where(row_session == b, product, score)
        cached[pl.ds(h * GROUP * per_shard, GROUP * per_shard)] = score

    parts = []
    for i, bias in enumerate((kb, vb)):
        part_copies[i].wait()
        whole = (own_part[i] + part_in[i] + bias[...]).astype(BF16)
        for h in range(kv_heads):
            parts.append(whole[:, h * HEAD : (h + 1) * HEAD])
            parts.append(jnp.zeros((lanes - rows, HEAD), BF16))
    table = jnp.concatenate(parts, axis=0)
    slotted = jnp.dot(onehot[...], table, preferred_element_type=F32).astype(BF16)
    send[...] = slotted.reshape(send.shape)

    pl.semaphore_wait(know3, len(group))
    here = column * NZ + z
    for dz in (4, 3, 5, 2, 6, 1, 7, 0):
        for dg in (1, 0):
            for dy in (2, 1, 3, 0):
                for dc in (0, 1):
                    if dg or dz or dy or dc:
                        device = turned(dg, dz, dy, dc)
                        to = device[0] * (NZ * NY * NC) + device[1]
                        pltpu.make_async_remote_copy(
                            send.at[to], recv.at[here], sem_data.at[0], sem_data.at[1], device_id=device,
                            device_id_type=MESH,
                        ).start()
    recv[here] = send[me]

    some = pl.ds(0, 15)
    pltpu.make_async_remote_copy(
        all_tok.at[some], all_tok.at[some], sem_all.at[0], sem_all.at[1], device_id=other, device_id_type=MESH
    ).wait()
    came = all_tok[...].reshape(PARTS, lanes)
    came_block = jnp.floor(came * 0.125)
    mine = came_block == jnp.full((1, 1), me, jnp.int32).astype(F32)
    upto = jnp.where(sub_i <= lane_i, 1.0, 0.0).astype(BF16)
    rank = jnp.dot(jnp.where(mine, 1.0, 0.0).astype(BF16), upto, preferred_element_type=F32)
    name = jnp.where(mine, came - came_block * 8.0 + 1.0, 0.0)
    first = jnp.sum(jnp.where(rank == 1.0, name, 0.0), axis=1, keepdims=True)
    second = jnp.sum(jnp.where(rank == 2.0, name, 0.0), axis=1, keepdims=True)
    names = jnp.where(lax.rem(lane_i // 4, 2) == 0, first, second)
    names = jnp.where(lane_i // 8 == lax.rem(sub_i, 16), names, 0.0)
    names = [jnp.sum(names[16 * i : 16 * i + 16], axis=0, keepdims=True) for i in range(8)]
    ids_row = jnp.concatenate(names, axis=1)

    everyone = pl.ds(0, PARTS - 1)
    pltpu.make_async_remote_copy(
        send.at[everyone], recv.at[everyone], sem_data.at[0], sem_data.at[1], device_id=other, device_id_type=MESH
    ).wait()
    fresh_rows = recv[...].reshape(PARTS * 8, HEAD)
    fresh = lax.dot_general(stacked, fresh_rows, (((1,), (1,)), ((), ())), preferred_element_type=F32) * scale
    shape = fresh.shape
    row_i = lax.broadcasted_iota(jnp.int32, shape, 0)
    col_i = lax.broadcasted_iota(jnp.int32, shape, 1)
    match = (ids_row == (lax.rem(row_i, per_shard) + 1).astype(F32)) & (
        lax.rem(col_i, 4) == row_i // (GROUP * per_shard)
    )
    fresh = jnp.where(match, fresh, -jnp.inf)
    held = cached[...]
    largest = jnp.maximum(jnp.max(held, axis=1, keepdims=True), jnp.max(fresh, axis=1, keepdims=True))
    held_exp = jnp.exp(held - largest)
    fresh_exp = jnp.exp(fresh - largest)
    total = jnp.sum(held_exp, axis=1, keepdims=True) + jnp.sum(fresh_exp, axis=1, keepdims=True)
    inverse_total = 1.0 / total
    held_weights = held_exp * inverse_total
    fresh_weights = pltpu.roll(fresh_exp * inverse_total, 2, 1).astype(BF16)
    result = jnp.dot(fresh_weights, fresh_rows, preferred_element_type=F32)
    for h in range(kv_heads):
        part = result[h * GROUP * per_shard : (h + 1) * GROUP * per_shard]
        mine = held_weights[h * GROUP * per_shard : (h + 1) * GROUP * per_shard]
        for b in range(per_shard):
            only = jnp.where(row_session == b, mine, 0.0).astype(BF16)
            part = part + jnp.dot(only, cv[b, :, pl.ds(h * HEAD, HEAD)], preferred_element_type=F32)
        for i in range(GROUP):
            out_ref[:, pl.ds((h * GROUP + i) * HEAD, HEAD)] = part[
                i * per_shard : (i + 1) * per_shard
            ].astype(BF16)


def local(
    frames, token_session, ln_gain, w_key, w_value, k_bias, v_bias, queries, cache_key, cache_value, cache_start,
    cache_len,
):
    rows, depth = frames.shape
    half = k_bias.shape[0]
    row = lambda a: a.reshape(1, -1)
    anywhere = pl.BlockSpec(memory_space=pltpu.HBM)
    dma = pltpu.SemaphoreType.DMA
    regular = pltpu.SemaphoreType.REGULAR
    vm = pltpu.VMEM
    return pl.pallas_call(
        kernel,
        out_shape=jax.ShapeDtypeStruct(queries.shape, BF16),
        in_specs=[anywhere] * 12,
        out_specs=pl.BlockSpec(memory_space=pltpu.VMEM),
        scratch_shapes=[
            vm((1, rows), jnp.int32), vm((rows, depth), BF16), vm((1, depth), F32), vm((4, depth, half), BF16),
            vm((1, half), F32), vm((1, half), F32), vm(queries.shape, BF16), vm(cache_key.shape, BF16),
            vm(cache_value.shape, BF16), pltpu.SMEM((8,), jnp.int32), pltpu.SMEM((8,), jnp.int32),
            vm((rows, depth), BF16), vm((1, 128), F32), vm((1, 128), F32), vm((2, rows, half), F32),
            vm((2, rows, half), F32), vm((2, rows, half), F32), vm((PARTS * 8, 512), BF16),
            vm((PARTS, 8, HEAD), BF16), vm((PARTS, 8, HEAD), BF16), vm((NZ, 1, 128), F32), vm((16, NZ, 1, 128), F32),
            vm((128, 128), F32),
            dma((16,)), dma((4,)), dma((2,)), dma((2,)), dma((2,)), dma((2,)), dma((2,)), dma((2,)),
            regular, regular, regular,
        ],
        compiler_params=pltpu.CompilerParams(
            collective_id=0, has_side_effects=True, vmem_limit_bytes=67_000_000
        ),
        name="frame_attention",
    )(
        row(token_session), frames, row(ln_gain), w_key, w_value, row(k_bias), row(v_bias), queries, cache_key,
        cache_value, cache_start, cache_len,
    )


def solution(mesh):
    rows = ("grp", "seq")
    return jax.shard_map(
        local,
        mesh=mesh,
        in_specs=(
            P(rows, "mp"), P(rows), P("mp"), P("mp", None), P("mp", None), P("mp"), P("mp"), P(rows, "mp"),
            P(rows, None, "mp"), P(rows, None, "mp"), P(rows), P(rows),
        ),
        out_specs=P(rows, "mp"),
        check_vma=False,
    )
```

```python
import functools

import jax
import jax.numpy as jnp
from jax import lax
from jax.experimental import pallas as pl
from jax.experimental.pallas import tpu as pltpu
from jax.sharding import PartitionSpec as P

HEAD = 128
GROUP = 8
EPSILON = 1e-6
MESH = pl.DeviceIdType.MESH

NZ, NY, NC, NG = 8, 4, 2, 2
PARTS = NG * NZ * NY * NC
F32 = jnp.float32
BF16 = jnp.bfloat16


def kernel(
    tok_hbm, frames_hbm, gain_hbm, wk_hbm, wv_hbm, kb_hbm, vb_hbm, q_hbm, ck_hbm, cv_hbm, start_hbm, len_hbm,
    out_ref,
    tok, frames, gain, weights, kb, vb, q, ck, cv, start, length,
    normed, square_out, square_in, part_out, part_in, own_part, onehot, send, recv, line_tok, all_tok, cached,
    sem_in, sem_w, sem_sq, sem_part_s, sem_part_r, sem_data_s, sem_data_r, sem_line, sem_all, know1, know2, know3,
):
    g, s, m = lax.axis_index("grp"), lax.axis_index("seq"), lax.axis_index("mp")
    core, y, z = lax.rem(s, NC), lax.rem(s // NC, NY), s // (NC * NY)
    me = g * (NZ * NY * NC) + s
    column = (g * NY + y) * NC + core
    rows, depth = frames.shape
    half = kb.shape[1]
    at_g = [g, 1 - g]
    at_z = [z] + [lax.rem(z + d, NZ) * (NY * NC) for d in range(1, NZ)]
    at_z[0] = z * (NY * NC)
    at_y = [y * NC] + [lax.rem(y + d, NY) * NC for d in range(1, NY)]
    at_core = [core, 1 - core]
    at_yc = [[at_y[dy] + at_core[dc] for dc in range(NC)] for dy in range(NY)]

    def turned(dg, dz, dy, dc):
        return (at_g[dg], at_z[dz] + at_yc[dy][dc], m)

    other = (g, s, 1 - m)

    def tell(sem, devices):
        for device in devices:
            pl.semaphore_signal(sem, inc=1, device_id=device, device_id_type=MESH)

    barrier = pltpu.get_barrier_semaphore()
    far_core = at_z[0] + at_yc[0][1]
    near = [
        other, (1 - g, s, 1 - m), (g, far_core, 1 - m), (1 - g, far_core, 1 - m), (g, far_core, m),
        turned(0, 1, 0, 0), turned(0, NZ - 1, 0, 0), turned(0, 0, 1, 0), turned(0, 0, NY - 1, 0),
    ]
    tell(barrier, near)

    chunk = 32
    loads = [
        pltpu.make_async_copy(
            frames_hbm.at[pl.ds(i * chunk, chunk)], frames.at[pl.ds(i * chunk, chunk)], sem_in.at[i]
        )
        for i in range(rows // chunk)
    ]
    n = len(loads)
    gain_load = pltpu.make_async_copy(gain_hbm, gain, sem_in.at[n])
    tok_load = pltpu.make_async_copy(tok_hbm, tok, sem_in.at[n + 1])
    small = [
        pltpu.make_async_copy(kb_hbm, kb, sem_in.at[n + 2]),
        pltpu.make_async_copy(vb_hbm, vb, sem_in.at[n + 3]),
    ]
    late = [
        pltpu.make_async_copy(q_hbm, q, sem_in.at[n + 4]),
        pltpu.make_async_copy(ck_hbm, ck, sem_in.at[n + 5]),
        pltpu.make_async_copy(cv_hbm, cv, sem_in.at[n + 6]),
        pltpu.make_async_copy(start_hbm, start, sem_in.at[n + 7]),
        pltpu.make_async_copy(len_hbm, length, sem_in.at[n + 8]),
    ]
    for load in loads:
        load.start()
    gain_load.start()
    tok_load.start()
    weight_loads = []
    for i, (source, side) in enumerate(((wk_hbm, 1 - m), (wv_hbm, 1 - m), (wk_hbm, m), (wv_hbm, m))):
        load = pltpu.make_async_copy(
            source.at[:, pl.ds(pl.multiple_of(side * half, half), half)], weights.at[i], sem_w.at[i]
        )
        load.start()
        weight_loads.append(load)
    for load in small + late:
        load.start()

    lanes = 128
    square_out[...] = jnp.zeros_like(square_out)
    sums = []
    for i, load in enumerate(loads):
        load.wait()
        total = jnp.zeros((chunk, lanes), F32)
        for j in range(depth // lanes):
            x = frames[pl.ds(i * chunk, chunk), pl.ds(j * lanes, lanes)].astype(F32)
            total = total + x * x
        sums.append(total)
    sums.append(jnp.zeros((lanes - rows, lanes), F32))
    own_squares = jnp.sum(jnp.concatenate(sums, axis=0).T, axis=0, keepdims=True)
    square_out[...] = own_squares
    pl.semaphore_wait(barrier, len(near))
    square_copy = pltpu.make_async_remote_copy(
        square_out, square_in, sem_sq.at[0], sem_sq.at[1], device_id=other, device_id_type=MESH
    )
    square_copy.start()
    tell(know1, [turned(0, 1, 0, 0), turned(0, NZ - 1, 0, 0), turned(0, 0, 1, 0), turned(0, 0, NY - 1, 0), other])

    tok_load.wait()
    padded = jnp.concatenate([tok[...].astype(F32), jnp.full((1, lanes - rows), -8.0 * PARTS, F32)], axis=1)
    line_tok[z] = padded
    row_at = lax.broadcasted_iota(jnp.int32, (1, lanes), 1)
    block = jnp.floor(padded * 0.125)
    block_here = jnp.broadcast_to(block, (lanes, lanes))
    lane_i = lax.broadcasted_iota(jnp.int32, (lanes, lanes), 1)
    sub_i = lax.broadcasted_iota(jnp.int32, (lanes, lanes), 0)
    before = (block_here.T == block_here) & (sub_i < lane_i)
    rank = jnp.sum(before.astype(F32), axis=0, keepdims=True)
    slot = jnp.where(row_at < rows, block * 2.0 + rank, -1.0)
    slot_here = jnp.broadcast_to(slot, (lanes, lanes))
    for p in range(4):
        hit = slot_here == (sub_i // 2 + p * 64).astype(F32)
        for h in range(2):
            onehot[pl.ds(p * lanes, lanes), pl.ds(h * lanes, lanes)] = jnp.where(
                hit & (lax.rem(sub_i, 2) == h), 1.0, 0.0
            ).astype(BF16)

    pl.semaphore_wait(know1, 5)
    line = [turned(0, 0, d, 0) for d in range(1, NY)]
    tell(know2, [turned(0, 2, 0, 0), turned(0, NZ - 2, 0, 0)] + line)

    gain_load.wait()
    square_copy.wait()
    squares = square_out[...] + square_in[...]
    inverse = lax.rsqrt(squares / (2 * depth) + EPSILON)
    inverse = jnp.broadcast_to(inverse, (lanes, lanes)).T[:rows]
    for j in range(depth // lanes):
        cols = pl.ds(j * lanes, lanes)
        normed[:, cols] = (frames[:, cols].astype(F32) * inverse * gain[:, cols]).astype(BF16)

    pl.semaphore_wait(know2, 5)
    group = [
        turned(dg, 0, dy, dc) for dg in range(NG) for dy in range(NY) for dc in range(NC) if dg or dy or dc
    ]
    tell(know3, group)
    for d in range(1, NZ):
        pltpu.make_async_remote_copy(
            line_tok.at[z], line_tok.at[z], sem_line.at[0], sem_line.at[1], device_id=turned(0, d, 0, 0), device_id_type=MESH
        ).start()

    part_copies = []
    for i in range(4):
        weight_loads[i].wait()
        product = jnp.dot(normed[...], weights[i], preferred_element_type=F32)
        if i < 2:
            part_out[i] = product
            copy = pltpu.make_async_remote_copy(
                part_out.at[i], part_in.at[i], sem_part_s.at[i], sem_part_r.at[i], device_id=other, device_id_type=MESH
            )
            copy.start()
            part_copies.append(copy)
        else:
            own_part[i - 2] = product
    for load in small + late:
        load.wait()

    heads = q.shape[1] // HEAD
    kv_heads = heads // GROUP
    per_shard = q.shape[0]
    stacked = jnp.concatenate([q[:, pl.ds(i * HEAD, HEAD)] for i in range(heads)], axis=0)
    scale = HEAD**-0.5
    window = ck.shape[1]
    slots = lax.broadcasted_iota(jnp.int32, (1, window), 1)
    row_session = lax.broadcasted_iota(jnp.int32, (GROUP * per_shard, lanes), 0)
    row_session = lax.rem(row_session, per_shard)
    for h in range(kv_heads):
        queries = stacked[h * GROUP * per_shard : (h + 1) * GROUP * per_shard]
        score = jnp.zeros((GROUP * per_shard, window), F32)
        for b in range(per_shard):
            keys = ck[b, :, pl.ds(h * HEAD, HEAD)]
            product = lax.dot_general(queries, keys, (((1,), (1,)), ((), ())), preferred_element_type=F32) * scale
            live = lax.rem(slots - start[b] + window, window) < length[b]
            product = jnp.where(live, product, -jnp.inf)
            score = jnp.where(row_session == b, product, score)
        cached[pl.ds(h * GROUP * per_shard, GROUP * per_shard)] = score

    here = column * NZ + z
    peers = [
        (dg, dz, dy, dc)
        for dz in (4, 3, 5, 2, 6, 1, 7, 0) for dg in (1, 0) for dy in (2, 1, 3, 0) for dc in (0, 1)
        if dg or dz or dy or dc
    ]
    for i, bias in enumerate((kb, vb)):
        part_copies[i].wait()
        whole = (own_part[i] + part_in[i] + bias[...]).astype(BF16)
        parts = []
        for h in range(kv_heads):
            parts.append(whole[:, h * HEAD : (h + 1) * HEAD])
            parts.append(jnp.zeros((lanes - rows, HEAD), BF16))
        table = jnp.concatenate(parts, axis=0)
        slotted = jnp.dot(onehot[...], table, preferred_element_type=F32).astype(BF16)
        send[i] = slotted.reshape(PARTS, 4, HEAD)
        if i == 0:
            pl.semaphore_wait(know3, len(group))
        for turn in peers:
            device = turned(*turn)
            to = device[0] * (NZ * NY * NC) + device[1]
            pltpu.make_async_remote_copy(
                send.at[i, to], recv.at[i, here], sem_data_s.at[i], sem_data_r.at[i], device_id=device,
                device_id_type=MESH,
            ).start()
        recv[i, here] = send[i, me]
        if i == 0:
            some = pl.ds(0, NZ - 1)
            pltpu.make_async_remote_copy(
                line_tok.at[some], line_tok.at[some], sem_line.at[0], sem_line.at[1], device_id=other, device_id_type=MESH
            ).wait()
            for device in group:
                pltpu.make_async_remote_copy(
                    line_tok, all_tok.at[column], sem_all.at[0], sem_all.at[1], device_id=device, device_id_type=MESH
                ).start()
            all_tok[column] = line_tok[...]

    some = pl.ds(0, 15)
    pltpu.make_async_remote_copy(
        all_tok.at[some], all_tok.at[some], sem_all.at[0], sem_all.at[1], device_id=other, device_id_type=MESH
    ).wait()
    came = all_tok[...].reshape(PARTS, lanes)
    came_block = jnp.floor(came * 0.125)
    mine = came_block == jnp.full((1, 1), me, jnp.int32).astype(F32)
    upto = jnp.where(sub_i <= lane_i, 1.0, 0.0).astype(BF16)
    rank = jnp.dot(jnp.where(mine, 1.0, 0.0).astype(BF16), upto, preferred_element_type=F32)
    name = jnp.where(mine, came - came_block * 8.0 + 1.0, 0.0)
    first = jnp.sum(jnp.where(rank == 1.0, name, 0.0), axis=1, keepdims=True)
    second = jnp.sum(jnp.where(rank == 2.0, name, 0.0), axis=1, keepdims=True)
    names = jnp.where(lax.rem(lane_i // 2, 2) == 0, first, second)
    names = jnp.where(lane_i // 4 == lax.rem(sub_i, 32), names, 0.0)
    names = [jnp.sum(names[32 * i : 32 * i + 32], axis=0, keepdims=True) for i in range(4)]
    ids_row = jnp.concatenate(names, axis=1)

    def arrived(i):
        everyone = pl.ds(0, PARTS - 1)
        pltpu.make_async_remote_copy(
            send.at[i, everyone], recv.at[i, everyone], sem_data_s.at[i], sem_data_r.at[i], device_id=other,
            device_id_type=MESH,
        ).wait()
        return recv[i].reshape(PARTS * 4, HEAD)

    fresh = lax.dot_general(stacked, arrived(0), (((1,), (1,)), ((), ())), preferred_element_type=F32) * scale
    shape = fresh.shape
    row_i = lax.broadcasted_iota(jnp.int32, shape, 0)
    col_i = lax.broadcasted_iota(jnp.int32, shape, 1)
    match = (ids_row == (lax.rem(row_i, per_shard) + 1).astype(F32)) & (
        lax.rem(col_i, 2) == row_i // (GROUP * per_shard)
    )
    fresh = jnp.where(match, fresh, -jnp.inf)
    held = cached[...]
    largest = jnp.maximum(jnp.max(held, axis=1, keepdims=True), jnp.max(fresh, axis=1, keepdims=True))
    held_exp = jnp.exp(held - largest)
    fresh_exp = jnp.exp(fresh - largest)
    total = jnp.sum(held_exp, axis=1, keepdims=True) + jnp.sum(fresh_exp, axis=1, keepdims=True)
    inverse_total = 1.0 / total
    held_weights = held_exp * inverse_total
    fresh_weights = (fresh_exp * inverse_total).astype(BF16)
    held_terms = []
    for h in range(kv_heads):
        mine = held_weights[h * GROUP * per_shard : (h + 1) * GROUP * per_shard]
        part = jnp.zeros((GROUP * per_shard, HEAD), F32)
        for b in range(per_shard):
            only = jnp.where(row_session == b, mine, 0.0).astype(BF16)
            part = part + jnp.dot(only, cv[b, :, pl.ds(h * HEAD, HEAD)], preferred_element_type=F32)
        held_terms.append(part)
    held_terms = jnp.concatenate(held_terms, axis=0)

    result = held_terms + jnp.dot(fresh_weights, arrived(1), preferred_element_type=F32)
    for i in range(heads):
        out_ref[:, pl.ds(i * HEAD, HEAD)] = result[i * per_shard : (i + 1) * per_shard].astype(BF16)


def local(
    frames, token_session, ln_gain, w_key, w_value, k_bias, v_bias, queries, cache_key, cache_value, cache_start,
    cache_len,
):
    rows, depth = frames.shape
    half = k_bias.shape[0]
    row = lambda a: a.reshape(1, -1)
    anywhere = pl.BlockSpec(memory_space=pltpu.HBM)
    dma = pltpu.SemaphoreType.DMA
    regular = pltpu.SemaphoreType.REGULAR
    vm = pltpu.VMEM
    return pl.pallas_call(
        kernel,
        out_shape=jax.ShapeDtypeStruct(queries.shape, BF16),
        in_specs=[anywhere] * 12,
        out_specs=pl.BlockSpec(memory_space=pltpu.VMEM),
        scratch_shapes=[
            vm((1, rows), jnp.int32), vm((rows, depth), BF16), vm((1, depth), F32), vm((4, depth, half), BF16),
            vm((1, half), F32), vm((1, half), F32), vm(queries.shape, BF16), vm(cache_key.shape, BF16),
            vm(cache_value.shape, BF16), pltpu.SMEM((8,), jnp.int32), pltpu.SMEM((8,), jnp.int32),
            vm((rows, depth), BF16), vm((1, 128), F32), vm((1, 128), F32), vm((2, rows, half), F32),
            vm((2, rows, half), F32), vm((2, rows, half), F32), vm((PARTS * 4, 256), BF16),
            vm((2, PARTS, 4, HEAD), BF16), vm((2, PARTS, 4, HEAD), BF16), vm((NZ, 1, 128), F32), vm((16, NZ, 1, 128), F32),
            vm((128, 128), F32),
            dma((16,)), dma((4,)), dma((2,)), dma((2,)), dma((2,)), dma((2,)), dma((2,)), dma((2,)), dma((2,)),
            regular, regular, regular,
        ],
        compiler_params=pltpu.CompilerParams(
            collective_id=0, has_side_effects=True, vmem_limit_bytes=67_000_000
        ),
        name="frame_attention",
    )(
        row(token_session), frames, row(ln_gain), w_key, w_value, row(k_bias), row(v_bias), queries, cache_key,
        cache_value, cache_start, cache_len,
    )


def solution(mesh):
    rows = ("grp", "seq")
    return jax.shard_map(
        local,
        mesh=mesh,
        in_specs=(
            P(rows, "mp"), P(rows), P("mp"), P("mp", None), P("mp", None), P("mp"), P("mp"), P(rows, "mp"),
            P(rows, None, "mp"), P(rows, None, "mp"), P(rows), P(rows),
        ),
        out_specs=P(rows, "mp"),
        check_vma=False,
    )
```

```python
import functools

import jax
import jax.numpy as jnp
from jax import lax
from jax.experimental import pallas as pl
from jax.experimental.pallas import tpu as pltpu
from jax.sharding import PartitionSpec as P

HEAD = 128
GROUP = 8
EPSILON = 1e-6
MESH = pl.DeviceIdType.MESH

NZ, NY, NC, NG = 8, 4, 2, 2
PARTS = NG * NZ * NY * NC
F32 = jnp.float32
BF16 = jnp.bfloat16


def kernel(
    tok_hbm, frames_hbm, gain_hbm, wk_hbm, wv_hbm, kb_hbm, vb_hbm, q_hbm, ck_hbm, cv_hbm, start_hbm, len_hbm,
    out_ref,
    tok, frames, gain, weights, kb, vb, q, ck, cv, start, length,
    normed, square_out, square_in, part_out, part_in, own_part, onehot, send, recv, line_tok, all_tok, cached,
    sem_in, sem_w, sem_sq, sem_part_s, sem_part_r, sem_data_s, sem_data_r, sem_line, sem_all, know1, know2, know3,
):
    g, s, m = lax.axis_index("grp"), lax.axis_index("seq"), lax.axis_index("mp")
    core, y, z = lax.rem(s, NC), lax.rem(s // NC, NY), s // (NC * NY)
    me = g * (NZ * NY * NC) + s
    column = (g * NY + y) * NC + core
    rows, depth = frames.shape
    half = kb.shape[1]
    at_g = [g, 1 - g]
    at_z = [z] + [lax.rem(z + d, NZ) * (NY * NC) for d in range(1, NZ)]
    at_z[0] = z * (NY * NC)
    at_y = [y * NC] + [lax.rem(y + d, NY) * NC for d in range(1, NY)]
    at_core = [core, 1 - core]
    at_yc = [[at_y[dy] + at_core[dc] for dc in range(NC)] for dy in range(NY)]

    def turned(dg, dz, dy, dc):
        return (at_g[dg], at_z[dz] + at_yc[dy][dc], m)

    other = (g, s, 1 - m)

    def tell(sem, devices):
        for device in devices:
            pl.semaphore_signal(sem, inc=1, device_id=device, device_id_type=MESH)

    barrier = pltpu.get_barrier_semaphore()
    far_core = at_z[0] + at_yc[0][1]
    near = [
        other, (1 - g, s, 1 - m), (g, far_core, 1 - m), (1 - g, far_core, 1 - m), (g, far_core, m),
        turned(0, 1, 0, 0), turned(0, NZ - 1, 0, 0), turned(0, 0, 1, 0), turned(0, 0, NY - 1, 0),
    ]
    tell(barrier, near)

    chunk = 32
    loads = [
        pltpu.make_async_copy(
            frames_hbm.at[pl.ds(i * chunk, chunk)], frames.at[pl.ds(i * chunk, chunk)], sem_in.at[i]
        )
        for i in range(rows // chunk)
    ]
    n = len(loads)
    gain_load = pltpu.make_async_copy(gain_hbm, gain, sem_in.at[n])
    tok_load = pltpu.make_async_copy(tok_hbm, tok, sem_in.at[n + 1])
    small = [
        pltpu.make_async_copy(kb_hbm, kb, sem_in.at[n + 2]),
        pltpu.make_async_copy(vb_hbm, vb, sem_in.at[n + 3]),
    ]
    late = [
        pltpu.make_async_copy(q_hbm, q, sem_in.at[n + 4]),
        pltpu.make_async_copy(ck_hbm, ck, sem_in.at[n + 5]),
        pltpu.make_async_copy(cv_hbm, cv, sem_in.at[n + 6]),
        pltpu.make_async_copy(start_hbm, start, sem_in.at[n + 7]),
        pltpu.make_async_copy(len_hbm, length, sem_in.at[n + 8]),
    ]
    for load in loads:
        load.start()
    gain_load.start()
    tok_load.start()
    weight_loads = []
    for i, (source, side) in enumerate(((wk_hbm, 1 - m), (wv_hbm, 1 - m), (wk_hbm, m), (wv_hbm, m))):
        load = pltpu.make_async_copy(
            source.at[:, pl.ds(pl.multiple_of(side * half, half), half)], weights.at[i], sem_w.at[i]
        )
        load.start()
        weight_loads.append(load)
    for load in small + late:
        load.start()

    pl.semaphore_wait(barrier, len(near))
    tell(know1, [turned(0, 1, 0, 0), turned(0, NZ - 1, 0, 0), turned(0, 0, 1, 0), turned(0, 0, NY - 1, 0), other])

    lanes = 128
    square_out[...] = jnp.zeros_like(square_out)
    sums = []
    for i, load in enumerate(loads):
        load.wait()
        total = jnp.zeros((chunk, lanes), F32)
        for j in range(depth // lanes):
            x = frames[pl.ds(i * chunk, chunk), pl.ds(j * lanes, lanes)].astype(F32)
            total = total + x * x
        sums.append(total)
    sums.append(jnp.zeros((lanes - rows, lanes), F32))
    own_squares = jnp.sum(jnp.concatenate(sums, axis=0).T, axis=0, keepdims=True)
    square_out[...] = own_squares
    square_copy = pltpu.make_async_remote_copy(
        square_out, square_in, sem_sq.at[0], sem_sq.at[1], device_id=other, device_id_type=MESH
    )
    square_copy.start()
    pl.semaphore_wait(know1, 5)
    line = [turned(0, 0, d, 0) for d in range(1, NY)]
    tell(know2, [turned(0, 2, 0, 0), turned(0, NZ - 2, 0, 0)] + line)

    tok_load.wait()
    padded = jnp.concatenate([tok[...].astype(F32), jnp.full((1, lanes - rows), -8.0 * PARTS, F32)], axis=1)
    line_tok[z] = padded
    row_at = lax.broadcasted_iota(jnp.int32, (1, lanes), 1)
    block = jnp.floor(padded * 0.125)
    block_here = jnp.broadcast_to(block, (lanes, lanes))
    lane_i = lax.broadcasted_iota(jnp.int32, (lanes, lanes), 1)
    sub_i = lax.broadcasted_iota(jnp.int32, (lanes, lanes), 0)
    before = (block_here.T == block_here) & (sub_i < lane_i)
    rank = jnp.sum(before.astype(F32), axis=0, keepdims=True)
    slot = jnp.where(row_at < rows, block * 2.0 + rank, -1.0)
    slot_here = jnp.broadcast_to(slot, (lanes, lanes))
    for p in range(4):
        hit = slot_here == (sub_i // 2 + p * 64).astype(F32)
        for h in range(2):
            onehot[pl.ds(p * lanes, lanes), pl.ds(h * lanes, lanes)] = jnp.where(
                hit & (lax.rem(sub_i, 2) == h), 1.0, 0.0
            ).astype(BF16)

    pl.semaphore_wait(know2, 5)
    group = [
        turned(dg, 0, dy, dc) for dg in range(NG) for dy in range(NY) for dc in range(NC) if dg or dy or dc
    ]
    tell(know3, group)
    for d in range(1, NZ):
        pltpu.make_async_remote_copy(
            line_tok.at[z], line_tok.at[z], sem_line.at[0], sem_line.at[1], device_id=turned(0, d, 0, 0), device_id_type=MESH
        ).start()

    gain_load.wait()
    square_copy.wait()
    squares = square_out[...] + square_in[...]
    inverse = lax.rsqrt(squares / (2 * depth) + EPSILON)
    inverse = jnp.broadcast_to(inverse, (lanes, lanes)).T[:rows]
    step = 512
    first_product = jnp.zeros((rows, half), F32)
    weight_loads[0].wait()
    for j in range(depth // step):
        cols = pl.ds(j * step, step)
        chunk_normed = (frames[:, cols].astype(F32) * inverse[:, :1] * gain[:, cols]).astype(BF16)
        normed[:, cols] = chunk_normed
        first_product = first_product + jnp.dot(chunk_normed, weights[0, cols], preferred_element_type=F32)

    part_copies, top_copies = [], []
    split = part_out.shape[0] // 2
    width = half // split

    def share(product, i):
        for at in range(split):
            piece = product[:, at * width : (at + 1) * width]
            j = i * split + at
            part_out[j] = piece
            copy = pltpu.make_async_remote_copy(
                part_out.at[j], part_in.at[j], sem_part_s.at[j], sem_part_r.at[j], device_id=other, device_id_type=MESH
            )
            copy.start()
            part_copies.append(copy)

    share(first_product, 0)
    for i in range(1, 4):
        weight_loads[i].wait()
        product = jnp.dot(normed[...], weights[i], preferred_element_type=F32)
        if i < 2:
            share(product, i)
        else:
            for at in range(split):
                own_part[(i - 2) * split + at] = product[:, at * width : (at + 1) * width]
    for load in small + late:
        load.wait()

    heads = q.shape[1] // HEAD
    kv_heads = heads // GROUP
    per_shard = q.shape[0]
    stacked = jnp.concatenate([q[:, pl.ds(i * HEAD, HEAD)] for i in range(heads)], axis=0)
    scale = HEAD**-0.5
    window = ck.shape[1]
    slots = lax.broadcasted_iota(jnp.int32, (1, window), 1)
    row_session = lax.broadcasted_iota(jnp.int32, (GROUP * per_shard, lanes), 0)
    row_session = lax.rem(row_session, per_shard)
    for h in range(kv_heads):
        queries = stacked[h * GROUP * per_shard : (h + 1) * GROUP * per_shard]
        score = jnp.zeros((GROUP * per_shard, window), F32)
        for b in range(per_shard):
            keys = ck[b, :, pl.ds(h * HEAD, HEAD)]
            product = lax.dot_general(queries, keys, (((1,), (1,)), ((), ())), preferred_element_type=F32) * scale
            live = lax.rem(slots - start[b] + window, window) < length[b]
            product = jnp.where(live, product, -jnp.inf)
            score = jnp.where(row_session == b, product, score)
        cached[pl.ds(h * GROUP * per_shard, GROUP * per_shard)] = score

    here = column * NZ + z
    peers = [
        (dg, dz, dy, dc)
        for dz in (4, 3, 5, 2, 6, 1, 7, 0) for dg in (1, 0) for dy in (2, 1, 3, 0) for dc in (0, 1)
        if dg or dz or dy or dc
    ]
    for i in range(2 * split):
        bias = (kb, vb)[i // split][:, (i % split) * width : (i % split + 1) * width]
        part_copies[i].wait()
        whole = (own_part[i] + part_in[i] + bias).astype(BF16)
        parts = []
        for h in range(width // HEAD):
            parts.append(whole[:, h * HEAD : (h + 1) * HEAD])
            parts.append(jnp.zeros((lanes - rows, HEAD), BF16))
        table = jnp.concatenate(parts, axis=0)
        slotted = jnp.dot(onehot[...], table, preferred_element_type=F32).astype(BF16)
        send[i] = slotted.reshape(send.shape[1:])
        if i == 0:
            pl.semaphore_wait(know3, len(group))
        for turn in peers:
            device = turned(*turn)
            to = device[0] * (NZ * NY * NC) + device[1]
            pltpu.make_async_remote_copy(
                send.at[i, to], recv.at[i, here], sem_data_s.at[i], sem_data_r.at[i], device_id=device,
                device_id_type=MESH,
            ).start()
        recv[i, here] = send[i, me]
        if i == split - 1:
            some = pl.ds(0, NZ - 1)
            pltpu.make_async_remote_copy(
                line_tok.at[some], line_tok.at[some], sem_line.at[0], sem_line.at[1], device_id=other, device_id_type=MESH
            ).wait()
            for device in group:
                pltpu.make_async_remote_copy(
                    line_tok, all_tok.at[column], sem_all.at[0], sem_all.at[1], device_id=device, device_id_type=MESH
                ).start()
            all_tok[column] = line_tok[...]

    some = pl.ds(0, 15)
    pltpu.make_async_remote_copy(
        all_tok.at[some], all_tok.at[some], sem_all.at[0], sem_all.at[1], device_id=other, device_id_type=MESH
    ).wait()
    came = all_tok[...].reshape(PARTS, lanes)
    came_block = jnp.floor(came * 0.125)
    mine = came_block == jnp.full((1, 1), me, jnp.int32).astype(F32)
    upto = jnp.where(sub_i <= lane_i, 1.0, 0.0).astype(BF16)
    rank = jnp.dot(jnp.where(mine, 1.0, 0.0).astype(BF16), upto, preferred_element_type=F32)
    name = jnp.where(mine, came - came_block * 8.0 + 1.0, 0.0)
    first = jnp.sum(jnp.where(rank == 1.0, name, 0.0), axis=1, keepdims=True)
    second = jnp.sum(jnp.where(rank == 2.0, name, 0.0), axis=1, keepdims=True)
    names = jnp.where(lax.rem(lane_i // 2, 2) == 0, first, second)
    names = jnp.where(lane_i // 4 == lax.rem(sub_i, 32), names, 0.0)
    names = [jnp.sum(names[32 * i : 32 * i + 32], axis=0, keepdims=True) for i in range(4)]
    ids_row = jnp.concatenate(names, axis=1)

    def arrived(i):
        everyone = pl.ds(0, PARTS - 1)
        pltpu.make_async_remote_copy(
            send.at[i, everyone], recv.at[i, everyone], sem_data_s.at[i], sem_data_r.at[i], device_id=other,
            device_id_type=MESH,
        ).wait()
        return recv[i].reshape(PARTS * 4, HEAD)

    fresh = lax.dot_general(stacked, arrived(0), (((1,), (1,)), ((), ())), preferred_element_type=F32) * scale
    shape = fresh.shape
    row_i = lax.broadcasted_iota(jnp.int32, shape, 0)
    col_i = lax.broadcasted_iota(jnp.int32, shape, 1)
    match = (ids_row == (lax.rem(row_i, per_shard) + 1).astype(F32)) & (
        lax.rem(col_i, 2) == row_i // (GROUP * per_shard)
    )
    fresh = jnp.where(match, fresh, -jnp.inf)
    held = cached[...]
    largest = jnp.maximum(jnp.max(held, axis=1, keepdims=True), jnp.max(fresh, axis=1, keepdims=True))
    held_exp = jnp.exp(held - largest)
    fresh_exp = jnp.exp(fresh - largest)
    total = jnp.sum(held_exp, axis=1, keepdims=True) + jnp.sum(fresh_exp, axis=1, keepdims=True)
    inverse_total = 1.0 / total
    held_weights = held_exp * inverse_total
    fresh_weights = (fresh_exp * inverse_total).astype(BF16)
    held_terms = []
    for h in range(kv_heads):
        mine = held_weights[h * GROUP * per_shard : (h + 1) * GROUP * per_shard]
        part = jnp.zeros((GROUP * per_shard, HEAD), F32)
        for b in range(per_shard):
            only = jnp.where(row_session == b, mine, 0.0).astype(BF16)
            part = part + jnp.dot(only, cv[b, :, pl.ds(h * HEAD, HEAD)], preferred_element_type=F32)
        held_terms.append(part)
    held_terms = jnp.concatenate(held_terms, axis=0)

    result = held_terms + jnp.dot(fresh_weights, arrived(1), preferred_element_type=F32)
    for i in range(heads):
        out_ref[:, pl.ds(i * HEAD, HEAD)] = result[i * per_shard : (i + 1) * per_shard].astype(BF16)


def local(
    frames, token_session, ln_gain, w_key, w_value, k_bias, v_bias, queries, cache_key, cache_value, cache_start,
    cache_len,
):
    rows, depth = frames.shape
    half = k_bias.shape[0]
    row = lambda a: a.reshape(1, -1)
    anywhere = pl.BlockSpec(memory_space=pltpu.HBM)
    dma = pltpu.SemaphoreType.DMA
    regular = pltpu.SemaphoreType.REGULAR
    vm = pltpu.VMEM
    return pl.pallas_call(
        kernel,
        out_shape=pltpu.VMEM(queries.shape, BF16),
        in_specs=[anywhere] * 12,
        out_specs=pl.BlockSpec(memory_space=pltpu.VMEM),
        scratch_shapes=[
            vm((1, rows), jnp.int32), vm((rows, depth), BF16), vm((1, depth), F32), vm((4, depth, half), BF16),
            vm((1, half), F32), vm((1, half), F32), vm(queries.shape, BF16), vm(cache_key.shape, BF16),
            vm(cache_value.shape, BF16), pltpu.SMEM((8,), jnp.int32), pltpu.SMEM((8,), jnp.int32),
            vm((rows, depth), BF16), vm((1, 128), F32), vm((1, 128), F32), vm((2, rows, half), F32),
            vm((2, rows, half), F32), vm((2, rows, half), F32), vm((PARTS * 4, 256), BF16),
            vm((2, PARTS, 4, HEAD), BF16), vm((2, PARTS, 4, HEAD), BF16), vm((NZ, 1, 128), F32), vm((16, NZ, 1, 128), F32),
            vm((128, 128), F32),
            dma((16,)), dma((4,)), dma((2,)), dma((2,)), dma((2,)), dma((2,)), dma((2,)), dma((2,)), dma((2,)),
            regular, regular, regular,
        ],
        compiler_params=pltpu.CompilerParams(
            collective_id=0, has_side_effects=True, vmem_limit_bytes=66_900_000
        ),
        name="frame_attention",
    )(
        row(token_session), frames, row(ln_gain), w_key, w_value, row(k_bias), row(v_bias), queries, cache_key,
        cache_value, cache_start, cache_len,
    )


def solution(mesh):
    rows = ("grp", "seq")
    return jax.shard_map(
        local,
        mesh=mesh,
        in_specs=(
            P(rows, "mp"), P(rows), P("mp"), P("mp", None), P("mp", None), P("mp"), P("mp"), P(rows, "mp"),
            P(rows, None, "mp"), P(rows, None, "mp"), P(rows), P(rows),
        ),
        out_specs=P(rows, "mp"),
        check_vma=False,
    )
```

```python
import functools

import jax
import jax.numpy as jnp
from jax import lax
from jax.experimental import pallas as pl
from jax.experimental.pallas import tpu as pltpu
from jax.sharding import PartitionSpec as P

HEAD = 128
GROUP = 8
EPSILON = 1e-6
MESH = pl.DeviceIdType.MESH

NZ, NY, NC, NG = 8, 4, 2, 2
PARTS = NG * NZ * NY * NC
F32 = jnp.float32
BF16 = jnp.bfloat16


def kernel(
    tok_hbm, frames_hbm, gain_hbm, wk_hbm, wv_hbm, kb_hbm, vb_hbm, q_hbm, ck_hbm, cv_hbm, start_hbm, len_hbm,
    out_ref,
    tok, frames, gain, weights, kb, vb, q, ck, cv, start, length,
    normed, square_out, square_in, part_out, part_in, own_part, onehot, send, recv, line_tok, all_tok, cached,
    sem_in, sem_w, sem_sq, sem_part_s, sem_part_r, sem_data_s, sem_data_r, sem_line, sem_all, know1, know2,
):
    g, s, m = lax.axis_index("grp"), lax.axis_index("seq"), lax.axis_index("mp")
    core, y, z = lax.rem(s, NC), lax.rem(s // NC, NY), s // (NC * NY)
    me = g * (NZ * NY * NC) + s
    column = (g * NY + y) * NC + core
    rows, depth = frames.shape
    half = kb.shape[1]
    at_g = [g, 1 - g]
    at_z = [z] + [lax.rem(z + d, NZ) * (NY * NC) for d in range(1, NZ)]
    at_z[0] = z * (NY * NC)
    at_y = [y * NC] + [lax.rem(y + d, NY) * NC for d in range(1, NY)]
    at_core = [core, 1 - core]
    at_yc = [[at_y[dy] + at_core[dc] for dc in range(NC)] for dy in range(NY)]

    def turned(dg, dz, dy, dc):
        return (at_g[dg], at_z[dz] + at_yc[dy][dc], m)

    other = (g, s, 1 - m)

    def tell(sem, devices):
        for device in devices:
            pl.semaphore_signal(sem, inc=1, device_id=device, device_id_type=MESH)

    barrier = pltpu.get_barrier_semaphore()
    near = [other] + [turned(0, d, 0, 0) for d in (1, 2, NZ - 2, NZ - 1)]
    near += [turned(0, 0, dy, dc) for dy in range(NY) for dc in range(NC) if dy or dc]
    near += [turned(1, 0, 0, dc) for dc in range(NC)]
    tell(barrier, near)

    chunk = 32
    loads = [
        pltpu.make_async_copy(
            frames_hbm.at[pl.ds(i * chunk, chunk)], frames.at[pl.ds(i * chunk, chunk)], sem_in.at[i]
        )
        for i in range(rows // chunk)
    ]
    n = len(loads)
    gain_load = pltpu.make_async_copy(gain_hbm, gain, sem_in.at[n])
    tok_load = pltpu.make_async_copy(tok_hbm, tok, sem_in.at[n + 1])
    small = [
        pltpu.make_async_copy(kb_hbm, kb, sem_in.at[n + 2]),
        pltpu.make_async_copy(vb_hbm, vb, sem_in.at[n + 3]),
    ]
    late = [
        pltpu.make_async_copy(q_hbm, q, sem_in.at[n + 4]),
        pltpu.make_async_copy(ck_hbm, ck, sem_in.at[n + 5]),
        pltpu.make_async_copy(cv_hbm, cv, sem_in.at[n + 6]),
        pltpu.make_async_copy(start_hbm, start, sem_in.at[n + 7]),
        pltpu.make_async_copy(len_hbm, length, sem_in.at[n + 8]),
    ]
    for load in loads:
        load.start()
    gain_load.start()
    tok_load.start()
    weight_loads = []
    for i, (source, side) in enumerate(((wk_hbm, 1 - m), (wv_hbm, 1 - m), (wk_hbm, m), (wv_hbm, m))):
        load = pltpu.make_async_copy(
            source.at[:, pl.ds(pl.multiple_of(side * half, half), half)], weights.at[i], sem_w.at[i]
        )
        load.start()
        weight_loads.append(load)
    for load in small + late:
        load.start()

    lanes = 128
    square_out[...] = jnp.zeros_like(square_out)
    sums = []
    for i, load in enumerate(loads):
        load.wait()
        total = jnp.zeros((chunk, lanes), F32)
        for j in range(depth // lanes):
            x = frames[pl.ds(i * chunk, chunk), pl.ds(j * lanes, lanes)].astype(F32)
            total = total + x * x
        sums.append(total)
    sums.append(jnp.zeros((lanes - rows, lanes), F32))
    own_squares = jnp.sum(jnp.concatenate(sums, axis=0).T, axis=0, keepdims=True)
    square_out[...] = own_squares
    pl.semaphore_wait(barrier, len(near))
    square_copy = pltpu.make_async_remote_copy(
        square_out, square_in, sem_sq.at[0], sem_sq.at[1], device_id=other, device_id_type=MESH
    )
    square_copy.start()
    tell(know1, [turned(0, 2, 0, 0), turned(0, NZ - 2, 0, 0)] + [turned(0, 0, d, 0) for d in range(1, NY)])

    tok_load.wait()
    padded = jnp.concatenate([tok[...].astype(F32), jnp.full((1, lanes - rows), -8.0 * PARTS, F32)], axis=1)
    line_tok[z] = padded
    row_at = lax.broadcasted_iota(jnp.int32, (1, lanes), 1)
    block = jnp.floor(padded * 0.125)
    block_here = jnp.broadcast_to(block, (lanes, lanes))
    lane_i = lax.broadcasted_iota(jnp.int32, (lanes, lanes), 1)
    sub_i = lax.broadcasted_iota(jnp.int32, (lanes, lanes), 0)
    before = (block_here.T == block_here) & (sub_i < lane_i)
    rank = jnp.sum(before.astype(F32), axis=0, keepdims=True)
    slot = jnp.where(row_at < rows, block * 2.0 + rank, -1.0)
    slot_here = jnp.broadcast_to(slot, (lanes, lanes))
    for p in range(4):
        hit = slot_here == (sub_i // 2 + p * 64).astype(F32)
        for h in range(2):
            onehot[pl.ds(p * lanes, lanes), pl.ds(h * lanes, lanes)] = jnp.where(
                hit & (lax.rem(sub_i, 2) == h), 1.0, 0.0
            ).astype(BF16)

    pl.semaphore_wait(know1, 5)
    group = [
        turned(dg, 0, dy, dc) for dg in range(NG) for dy in range(NY) for dc in range(NC) if dg or dy or dc
    ]
    tell(know2, group)
    for d in range(1, NZ):
        pltpu.make_async_remote_copy(
            line_tok.at[z], line_tok.at[z], sem_line.at[0], sem_line.at[1], device_id=turned(0, d, 0, 0), device_id_type=MESH
        ).start()

    gain_load.wait()
    square_copy.wait()
    squares = square_out[...] + square_in[...]
    inverse = lax.rsqrt(squares / (2 * depth) + EPSILON)
    inverse = jnp.broadcast_to(inverse, (lanes, lanes)).T[:rows]
    step = 512
    first_product = jnp.zeros((rows, half), F32)
    weight_loads[0].wait()
    for j in range(depth // step):
        cols = pl.ds(j * step, step)
        chunk_normed = (frames[:, cols].astype(F32) * inverse[:, :1] * gain[:, cols]).astype(BF16)
        normed[:, cols] = chunk_normed
        first_product = first_product + jnp.dot(chunk_normed, weights[0, cols], preferred_element_type=F32)

    part_copies, top_copies = [], []
    split = part_out.shape[0] // 2
    width = half // split

    def share(product, i):
        for at in range(split):
            piece = product[:, at * width : (at + 1) * width]
            j = i * split + at
            part_out[j] = piece
            copy = pltpu.make_async_remote_copy(
                part_out.at[j], part_in.at[j], sem_part_s.at[j], sem_part_r.at[j], device_id=other, device_id_type=MESH
            )
            copy.start()
            part_copies.append(copy)

    share(first_product, 0)
    for i in range(1, 4):
        weight_loads[i].wait()
        product = jnp.dot(normed[...], weights[i], preferred_element_type=F32)
        if i < 2:
            share(product, i)
        else:
            for at in range(split):
                own_part[(i - 2) * split + at] = product[:, at * width : (at + 1) * width]
    for load in small + late:
        load.wait()

    heads = q.shape[1] // HEAD
    kv_heads = heads // GROUP
    per_shard = q.shape[0]
    stacked = jnp.concatenate([q[:, pl.ds(i * HEAD, HEAD)] for i in range(heads)], axis=0)
    scale = HEAD**-0.5
    window = ck.shape[1]
    slots = lax.broadcasted_iota(jnp.int32, (1, window), 1)
    row_session = lax.broadcasted_iota(jnp.int32, (GROUP * per_shard, lanes), 0)
    row_session = lax.rem(row_session, per_shard)
    for h in range(kv_heads):
        queries = stacked[h * GROUP * per_shard : (h + 1) * GROUP * per_shard]
        score = jnp.zeros((GROUP * per_shard, window), F32)
        for b in range(per_shard):
            keys = ck[b, :, pl.ds(h * HEAD, HEAD)]
            product = lax.dot_general(queries, keys, (((1,), (1,)), ((), ())), preferred_element_type=F32) * scale
            live = lax.rem(slots - start[b] + window, window) < length[b]
            product = jnp.where(live, product, -jnp.inf)
            score = jnp.where(row_session == b, product, score)
        cached[pl.ds(h * GROUP * per_shard, GROUP * per_shard)] = score

    some = pl.ds(0, NZ - 1)
    pltpu.make_async_remote_copy(
        line_tok.at[some], line_tok.at[some], sem_line.at[0], sem_line.at[1], device_id=other, device_id_type=MESH
    ).wait()
    for device in group:
        pltpu.make_async_remote_copy(
            line_tok, all_tok.at[column], sem_all.at[0], sem_all.at[1], device_id=device, device_id_type=MESH
        ).start()
    all_tok[column] = line_tok[...]

    here = column * NZ + z
    peers = [
        (dg, dz, dy, dc)
        for dz in (4, 3, 5, 2, 6, 1, 7, 0) for dg in (1, 0) for dy in (2, 1, 3, 0) for dc in (0, 1)
        if dg or dz or dy or dc
    ]
    for i in range(2 * split):
        bias = (kb, vb)[i // split][:, (i % split) * width : (i % split + 1) * width]
        part_copies[i].wait()
        whole = (own_part[i] + part_in[i] + bias).astype(BF16)
        parts = []
        for h in range(width // HEAD):
            parts.append(whole[:, h * HEAD : (h + 1) * HEAD])
            parts.append(jnp.zeros((lanes - rows, HEAD), BF16))
        table = jnp.concatenate(parts, axis=0)
        slotted = jnp.dot(onehot[...], table, preferred_element_type=F32).astype(BF16)
        send[i] = slotted.reshape(send.shape[1:])
        if i == 0:
            pl.semaphore_wait(know2, len(group))
        for turn in peers:
            device = turned(*turn)
            to = device[0] * (NZ * NY * NC) + device[1]
            pltpu.make_async_remote_copy(
                send.at[i, to], recv.at[i, here], sem_data_s.at[i], sem_data_r.at[i], device_id=device,
                device_id_type=MESH,
            ).start()
        recv[i, here] = send[i, me]

    some = pl.ds(0, 15)
    pltpu.make_async_remote_copy(
        all_tok.at[some], all_tok.at[some], sem_all.at[0], sem_all.at[1], device_id=other, device_id_type=MESH
    ).wait()
    came = all_tok[...].reshape(PARTS, lanes)
    came_block = jnp.floor(came * 0.125)
    mine = came_block == jnp.full((1, 1), me, jnp.int32).astype(F32)
    upto = jnp.where(sub_i <= lane_i, 1.0, 0.0).astype(BF16)
    rank = jnp.dot(jnp.where(mine, 1.0, 0.0).astype(BF16), upto, preferred_element_type=F32)
    name = jnp.where(mine, came - came_block * 8.0 + 1.0, 0.0)
    first = jnp.sum(jnp.where(rank == 1.0, name, 0.0), axis=1, keepdims=True)
    second = jnp.sum(jnp.where(rank == 2.0, name, 0.0), axis=1, keepdims=True)
    names = jnp.where(lax.rem(lane_i // 2, 2) == 0, first, second)
    names = jnp.where(lane_i // 4 == lax.rem(sub_i, 32), names, 0.0)
    names = [jnp.sum(names[32 * i : 32 * i + 32], axis=0, keepdims=True) for i in range(4)]
    ids_row = jnp.concatenate(names, axis=1)

    def arrived(i):
        everyone = pl.ds(0, PARTS - 1)
        pltpu.make_async_remote_copy(
            send.at[i, everyone], recv.at[i, everyone], sem_data_s.at[i], sem_data_r.at[i], device_id=other,
            device_id_type=MESH,
        ).wait()
        return recv[i].reshape(PARTS * 4, HEAD)

    fresh = lax.dot_general(stacked, arrived(0), (((1,), (1,)), ((), ())), preferred_element_type=F32) * scale
    shape = fresh.shape
    row_i = lax.broadcasted_iota(jnp.int32, shape, 0)
    col_i = lax.broadcasted_iota(jnp.int32, shape, 1)
    match = (ids_row == (lax.rem(row_i, per_shard) + 1).astype(F32)) & (
        lax.rem(col_i, 2) == row_i // (GROUP * per_shard)
    )
    fresh = jnp.where(match, fresh, -jnp.inf)
    held = cached[...]
    largest = jnp.maximum(jnp.max(held, axis=1, keepdims=True), jnp.max(fresh, axis=1, keepdims=True))
    held_exp = jnp.exp(held - largest)
    fresh_exp = jnp.exp(fresh - largest)
    total = jnp.sum(held_exp, axis=1, keepdims=True) + jnp.sum(fresh_exp, axis=1, keepdims=True)
    inverse_total = 1.0 / total
    held_weights = held_exp * inverse_total
    fresh_weights = (fresh_exp * inverse_total).astype(BF16)
    held_terms = []
    for h in range(kv_heads):
        mine = held_weights[h * GROUP * per_shard : (h + 1) * GROUP * per_shard]
        part = jnp.zeros((GROUP * per_shard, HEAD), F32)
        for b in range(per_shard):
            only = jnp.where(row_session == b, mine, 0.0).astype(BF16)
            part = part + jnp.dot(only, cv[b, :, pl.ds(h * HEAD, HEAD)], preferred_element_type=F32)
        held_terms.append(part)
    held_terms = jnp.concatenate(held_terms, axis=0)

    result = held_terms + jnp.dot(fresh_weights, arrived(1), preferred_element_type=F32)
    for i in range(heads):
        out_ref[:, pl.ds(i * HEAD, HEAD)] = result[i * per_shard : (i + 1) * per_shard].astype(BF16)


def local(
    frames, token_session, ln_gain, w_key, w_value, k_bias, v_bias, queries, cache_key, cache_value, cache_start,
    cache_len,
):
    rows, depth = frames.shape
    half = k_bias.shape[0]
    row = lambda a: a.reshape(1, -1)
    anywhere = pl.BlockSpec(memory_space=pltpu.HBM)
    dma = pltpu.SemaphoreType.DMA
    regular = pltpu.SemaphoreType.REGULAR
    vm = pltpu.VMEM
    return pl.pallas_call(
        kernel,
        out_shape=pltpu.VMEM(queries.shape, BF16),
        in_specs=[anywhere] * 12,
        out_specs=pl.BlockSpec(memory_space=pltpu.VMEM),
        scratch_shapes=[
            vm((1, rows), jnp.int32), vm((rows, depth), BF16), vm((1, depth), F32), vm((4, depth, half), BF16),
            vm((1, half), F32), vm((1, half), F32), vm(queries.shape, BF16), vm(cache_key.shape, BF16),
            vm(cache_value.shape, BF16), pltpu.SMEM((8,), jnp.int32), pltpu.SMEM((8,), jnp.int32),
            vm((rows, depth), BF16), vm((1, 128), F32), vm((1, 128), F32), vm((2, rows, half), F32),
            vm((2, rows, half), F32), vm((2, rows, half), F32), vm((PARTS * 4, 256), BF16),
            vm((2, PARTS, 4, HEAD), BF16), vm((2, PARTS, 4, HEAD), BF16), vm((NZ, 1, 128), F32), vm((16, NZ, 1, 128), F32),
            vm((128, 128), F32),
            dma((16,)), dma((4,)), dma((2,)), dma((2,)), dma((2,)), dma((2,)), dma((2,)), dma((2,)), dma((2,)),
            regular, regular,
        ],
        compiler_params=pltpu.CompilerParams(
            collective_id=0, has_side_effects=True, vmem_limit_bytes=66_900_000
        ),
        name="frame_attention",
    )(
        row(token_session), frames, row(ln_gain), w_key, w_value, row(k_bias), row(v_bias), queries, cache_key,
        cache_value, cache_start, cache_len,
    )


def solution(mesh):
    rows = ("grp", "seq")
    return jax.shard_map(
        local,
        mesh=mesh,
        in_specs=(
            P(rows, "mp"), P(rows), P("mp"), P("mp", None), P("mp", None), P("mp"), P("mp"), P(rows, "mp"),
            P(rows, None, "mp"), P(rows, None, "mp"), P(rows), P(rows),
        ),
        out_specs=P(rows, "mp"),
        check_vma=False,
    )
```

```python
import functools

import jax
import jax.numpy as jnp
from jax import lax
from jax.experimental import pallas as pl
from jax.experimental.pallas import tpu as pltpu
from jax.sharding import PartitionSpec as P

HEAD = 128
GROUP = 8
EPSILON = 1e-6
MESH = pl.DeviceIdType.MESH

NZ, NY, NC, NG = 8, 4, 2, 2
PARTS = NG * NZ * NY * NC
F32 = jnp.float32
BF16 = jnp.bfloat16


def kernel(
    tok_hbm, frames_hbm, gain_hbm, wk_hbm, wv_hbm, kb_hbm, vb_hbm, q_hbm, ck_hbm, cv_hbm, start_hbm, len_hbm,
    out_ref,
    tok, frames, gain, weights, kb, vb, q, ck, cv, start, length,
    normed, square_out, square_in, part_out, part_in, own_part, top_out, top_in, onehot, send, recv, line_tok, all_tok, cached,
    sem_in, sem_w, sem_sq, sem_part_s, sem_part_r, sem_top_s, sem_top_r, sem_data_s, sem_data_r, sem_line, sem_all, know1, know2,
):
    g, s, m = lax.axis_index("grp"), lax.axis_index("seq"), lax.axis_index("mp")
    core, y, z = lax.rem(s, NC), lax.rem(s // NC, NY), s // (NC * NY)
    me = g * (NZ * NY * NC) + s
    column = (g * NY + y) * NC + core
    rows, depth = frames.shape
    half = kb.shape[1]
    at_g = [g, 1 - g]
    at_z = [z] + [lax.rem(z + d, NZ) * (NY * NC) for d in range(1, NZ)]
    at_z[0] = z * (NY * NC)
    at_y = [y * NC] + [lax.rem(y + d, NY) * NC for d in range(1, NY)]
    at_core = [core, 1 - core]
    at_yc = [[at_y[dy] + at_core[dc] for dc in range(NC)] for dy in range(NY)]

    def turned(dg, dz, dy, dc):
        return (at_g[dg], at_z[dz] + at_yc[dy][dc], m)

    other = (g, s, 1 - m)

    def tell(sem, devices):
        for device in devices:
            pl.semaphore_signal(sem, inc=1, device_id=device, device_id_type=MESH)

    barrier = pltpu.get_barrier_semaphore()
    near = [other] + [turned(0, d, 0, 0) for d in (1, 2, NZ - 2, NZ - 1)]
    near += [turned(0, 0, dy, dc) for dy in range(NY) for dc in range(NC) if dy or dc]
    near += [turned(1, 0, 0, dc) for dc in range(NC)]
    tell(barrier, near)

    chunk = 32
    loads = [
        pltpu.make_async_copy(
            frames_hbm.at[pl.ds(i * chunk, chunk)], frames.at[pl.ds(i * chunk, chunk)], sem_in.at[i]
        )
        for i in range(rows // chunk)
    ]
    n = len(loads)
    gain_load = pltpu.make_async_copy(gain_hbm, gain, sem_in.at[n])
    tok_load = pltpu.make_async_copy(tok_hbm, tok, sem_in.at[n + 1])
    small = [
        pltpu.make_async_copy(kb_hbm, kb, sem_in.at[n + 2]),
        pltpu.make_async_copy(vb_hbm, vb, sem_in.at[n + 3]),
    ]
    late = [
        pltpu.make_async_copy(q_hbm, q, sem_in.at[n + 4]),
        pltpu.make_async_copy(ck_hbm, ck, sem_in.at[n + 5]),
        pltpu.make_async_copy(cv_hbm, cv, sem_in.at[n + 6]),
        pltpu.make_async_copy(start_hbm, start, sem_in.at[n + 7]),
        pltpu.make_async_copy(len_hbm, length, sem_in.at[n + 8]),
    ]
    for load in loads:
        load.start()
    gain_load.start()
    tok_load.start()
    weight_loads = []
    for i, (source, side) in enumerate(((wk_hbm, 1 - m), (wv_hbm, 1 - m), (wk_hbm, m), (wv_hbm, m))):
        load = pltpu.make_async_copy(
            source.at[:, pl.ds(pl.multiple_of(side * half, half), half)], weights.at[i], sem_w.at[i]
        )
        load.start()
        weight_loads.append(load)
    for load in small + late:
        load.start()

    lanes = 128
    square_out[...] = jnp.zeros_like(square_out)
    sums = []
    for i, load in enumerate(loads):
        load.wait()
        total = jnp.zeros((chunk, lanes), F32)
        for j in range(depth // lanes):
            x = frames[pl.ds(i * chunk, chunk), pl.ds(j * lanes, lanes)].astype(F32)
            total = total + x * x
        sums.append(total)
    sums.append(jnp.zeros((lanes - rows, lanes), F32))
    own_squares = jnp.sum(jnp.concatenate(sums, axis=0).T, axis=0, keepdims=True)
    square_out[...] = own_squares
    pl.semaphore_wait(barrier, len(near))
    square_copy = pltpu.make_async_remote_copy(
        square_out, square_in, sem_sq.at[0], sem_sq.at[1], device_id=other, device_id_type=MESH
    )
    square_copy.start()
    tell(know1, [turned(0, 2, 0, 0), turned(0, NZ - 2, 0, 0)] + [turned(0, 0, d, 0) for d in range(1, NY)])

    tok_load.wait()
    padded = jnp.concatenate([tok[...].astype(F32), jnp.full((1, lanes - rows), -8.0 * PARTS, F32)], axis=1)
    line_tok[z] = padded
    row_at = lax.broadcasted_iota(jnp.int32, (1, lanes), 1)
    block = jnp.floor(padded * 0.125)
    block_here = jnp.broadcast_to(block, (lanes, lanes))
    lane_i = lax.broadcasted_iota(jnp.int32, (lanes, lanes), 1)
    sub_i = lax.broadcasted_iota(jnp.int32, (lanes, lanes), 0)
    before = (block_here.T == block_here) & (sub_i < lane_i)
    rank = jnp.sum(before.astype(F32), axis=0, keepdims=True)
    slot = jnp.where(row_at < rows, block * 2.0 + rank, -1.0)
    slot_here = jnp.broadcast_to(slot, (lanes, lanes))
    for p in range(4):
        hit = slot_here == (sub_i // 2 + p * 64).astype(F32)
        for h in range(2):
            onehot[pl.ds(p * lanes, lanes), pl.ds(h * lanes, lanes)] = jnp.where(
                hit & (lax.rem(sub_i, 2) == h), 1.0, 0.0
            ).astype(BF16)

    pl.semaphore_wait(know1, 5)
    group = [
        turned(dg, 0, dy, dc) for dg in range(NG) for dy in range(NY) for dc in range(NC) if dg or dy or dc
    ]
    tell(know2, group)
    for d in range(1, NZ):
        pltpu.make_async_remote_copy(
            line_tok.at[z], line_tok.at[z], sem_line.at[0], sem_line.at[1], device_id=turned(0, d, 0, 0), device_id_type=MESH
        ).start()

    gain_load.wait()
    square_copy.wait()
    squares = square_out[...] + square_in[...]
    inverse = lax.rsqrt(squares / (2 * depth) + EPSILON)
    inverse = jnp.broadcast_to(inverse, (lanes, lanes)).T[:rows]
    step = 512
    first_product = jnp.zeros((rows, half), F32)
    weight_loads[0].wait()
    for j in range(depth // step):
        cols = pl.ds(j * step, step)
        chunk_normed = (frames[:, cols].astype(F32) * inverse[:, :1] * gain[:, cols]).astype(BF16)
        normed[:, cols] = chunk_normed
        first_product = first_product + jnp.dot(chunk_normed, weights[0, cols], preferred_element_type=F32)

    part_copies, top_copies = [], []
    split = part_out.shape[0] // 2
    width = half // split

    def share(product, i):
        for at in range(split):
            piece = product[:, at * width : (at + 1) * width]
            j = i * split + at
            biggest = jnp.maximum(jnp.max(jnp.abs(piece), axis=1, keepdims=True), 1e-30)
            part_out[j] = jnp.round(piece * (32767.0 / biggest)).astype(jnp.int32).astype(jnp.int16)
            tall = jnp.concatenate(
                [jnp.broadcast_to(biggest, (rows, lanes)), jnp.zeros((lanes - rows, lanes), F32)], axis=0
            )
            top_out[j] = tall.T[:1]
            copy = pltpu.make_async_remote_copy(
                part_out.at[j], part_in.at[j], sem_part_s.at[j], sem_part_r.at[j], device_id=other, device_id_type=MESH
            )
            copy.start()
            part_copies.append(copy)
            copy = pltpu.make_async_remote_copy(
                top_out.at[j], top_in.at[j], sem_top_s.at[j], sem_top_r.at[j], device_id=other, device_id_type=MESH
            )
            copy.start()
            top_copies.append(copy)

    share(first_product, 0)
    for i in range(1, 4):
        weight_loads[i].wait()
        product = jnp.dot(normed[...], weights[i], preferred_element_type=F32)
        if i < 2:
            share(product, i)
        else:
            for at in range(split):
                own_part[(i - 2) * split + at] = product[:, at * width : (at + 1) * width]
    for load in small + late:
        load.wait()

    heads = q.shape[1] // HEAD
    kv_heads = heads // GROUP
    per_shard = q.shape[0]
    stacked = jnp.concatenate([q[:, pl.ds(i * HEAD, HEAD)] for i in range(heads)], axis=0)
    scale = HEAD**-0.5
    window = ck.shape[1]
    slots = lax.broadcasted_iota(jnp.int32, (1, window), 1)
    row_session = lax.broadcasted_iota(jnp.int32, (GROUP * per_shard, lanes), 0)
    row_session = lax.rem(row_session, per_shard)
    for h in range(kv_heads):
        queries = stacked[h * GROUP * per_shard : (h + 1) * GROUP * per_shard]
        score = jnp.zeros((GROUP * per_shard, window), F32)
        for b in range(per_shard):
            keys = ck[b, :, pl.ds(h * HEAD, HEAD)]
            product = lax.dot_general(queries, keys, (((1,), (1,)), ((), ())), preferred_element_type=F32) * scale
            live = lax.rem(slots - start[b] + window, window) < length[b]
            product = jnp.where(live, product, -jnp.inf)
            score = jnp.where(row_session == b, product, score)
        cached[pl.ds(h * GROUP * per_shard, GROUP * per_shard)] = score

    some = pl.ds(0, NZ - 1)
    pltpu.make_async_remote_copy(
        line_tok.at[some], line_tok.at[some], sem_line.at[0], sem_line.at[1], device_id=other, device_id_type=MESH
    ).wait()
    for device in group:
        pltpu.make_async_remote_copy(
            line_tok, all_tok.at[column], sem_all.at[0], sem_all.at[1], device_id=device, device_id_type=MESH
        ).start()
    all_tok[column] = line_tok[...]

    here = column * NZ + z
    peers = [
        (dg, dz, dy, dc)
        for dz in (4, 3, 5, 2, 6, 1, 7, 0) for dg in (1, 0) for dy in (2, 1, 3, 0) for dc in (0, 1)
        if dg or dz or dy or dc
    ]
    for i in range(2 * split):
        bias = (kb, vb)[i // split][:, (i % split) * width : (i % split + 1) * width]
        part_copies[i].wait()
        top_copies[i].wait()
        top = jnp.broadcast_to(top_in[i], (lanes, lanes)).T[:rows, :1] * (1.0 / 32767.0)
        theirs = part_in[i].astype(jnp.int32).astype(F32) * top
        whole = (own_part[i] + theirs + bias).astype(BF16)
        parts = []
        for h in range(width // HEAD):
            parts.append(whole[:, h * HEAD : (h + 1) * HEAD])
            parts.append(jnp.zeros((lanes - rows, HEAD), BF16))
        table = jnp.concatenate(parts, axis=0)
        slotted = jnp.dot(onehot[...], table, preferred_element_type=F32).astype(BF16)
        send[i] = slotted.reshape(send.shape[1:])
        if i == 0:
            pl.semaphore_wait(know2, len(group))
        for turn in peers:
            device = turned(*turn)
            to = device[0] * (NZ * NY * NC) + device[1]
            pltpu.make_async_remote_copy(
                send.at[i, to], recv.at[i, here], sem_data_s.at[i], sem_data_r.at[i], device_id=device,
                device_id_type=MESH,
            ).start()
        recv[i, here] = send[i, me]

    some = pl.ds(0, 15)
    pltpu.make_async_remote_copy(
        all_tok.at[some], all_tok.at[some], sem_all.at[0], sem_all.at[1], device_id=other, device_id_type=MESH
    ).wait()
    came = all_tok[...].reshape(PARTS, lanes)
    came_block = jnp.floor(came * 0.125)
    mine = came_block == jnp.full((1, 1), me, jnp.int32).astype(F32)
    upto = jnp.where(sub_i <= lane_i, 1.0, 0.0).astype(BF16)
    rank = jnp.dot(jnp.where(mine, 1.0, 0.0).astype(BF16), upto, preferred_element_type=F32)
    name = jnp.where(mine, came - came_block * 8.0 + 1.0, 0.0)
    first = jnp.sum(jnp.where(rank == 1.0, name, 0.0), axis=1, keepdims=True)
    second = jnp.sum(jnp.where(rank == 2.0, name, 0.0), axis=1, keepdims=True)
    names = jnp.where(lax.rem(lane_i // 2, 2) == 0, first, second)
    names = jnp.where(lane_i // 4 == lax.rem(sub_i, 32), names, 0.0)
    names = [jnp.sum(names[32 * i : 32 * i + 32], axis=0, keepdims=True) for i in range(4)]
    ids_row = jnp.concatenate(names, axis=1)

    def arrived(i):
        everyone = pl.ds(0, PARTS - 1)
        pltpu.make_async_remote_copy(
            send.at[i, everyone], recv.at[i, everyone], sem_data_s.at[i], sem_data_r.at[i], device_id=other,
            device_id_type=MESH,
        ).wait()
        return recv[i].reshape(PARTS * 4, HEAD)

    fresh = lax.dot_general(stacked, arrived(0), (((1,), (1,)), ((), ())), preferred_element_type=F32) * scale
    shape = fresh.shape
    row_i = lax.broadcasted_iota(jnp.int32, shape, 0)
    col_i = lax.broadcasted_iota(jnp.int32, shape, 1)
    match = (ids_row == (lax.rem(row_i, per_shard) + 1).astype(F32)) & (
        lax.rem(col_i, 2) == row_i // (GROUP * per_shard)
    )
    fresh = jnp.where(match, fresh, -jnp.inf)
    held = cached[...]
    largest = jnp.maximum(jnp.max(held, axis=1, keepdims=True), jnp.max(fresh, axis=1, keepdims=True))
    held_exp = jnp.exp(held - largest)
    fresh_exp = jnp.exp(fresh - largest)
    total = jnp.sum(held_exp, axis=1, keepdims=True) + jnp.sum(fresh_exp, axis=1, keepdims=True)
    inverse_total = 1.0 / total
    held_weights = held_exp * inverse_total
    fresh_weights = (fresh_exp * inverse_total).astype(BF16)
    held_terms = []
    for h in range(kv_heads):
        mine = held_weights[h * GROUP * per_shard : (h + 1) * GROUP * per_shard]
        part = jnp.zeros((GROUP * per_shard, HEAD), F32)
        for b in range(per_shard):
            only = jnp.where(row_session == b, mine, 0.0).astype(BF16)
            part = part + jnp.dot(only, cv[b, :, pl.ds(h * HEAD, HEAD)], preferred_element_type=F32)
        held_terms.append(part)
    held_terms = jnp.concatenate(held_terms, axis=0)

    result = held_terms + jnp.dot(fresh_weights, arrived(1), preferred_element_type=F32)
    for i in range(heads):
        out_ref[:, pl.ds(i * HEAD, HEAD)] = result[i * per_shard : (i + 1) * per_shard].astype(BF16)


def local(
    frames, token_session, ln_gain, w_key, w_value, k_bias, v_bias, queries, cache_key, cache_value, cache_start,
    cache_len,
):
    rows, depth = frames.shape
    half = k_bias.shape[0]
    row = lambda a: a.reshape(1, -1)
    anywhere = pl.BlockSpec(memory_space=pltpu.HBM)
    dma = pltpu.SemaphoreType.DMA
    regular = pltpu.SemaphoreType.REGULAR
    vm = pltpu.VMEM
    return pl.pallas_call(
        kernel,
        out_shape=pltpu.VMEM(queries.shape, BF16),
        in_specs=[anywhere] * 12,
        out_specs=pl.BlockSpec(memory_space=pltpu.VMEM),
        scratch_shapes=[
            vm((1, rows), jnp.int32), vm((rows, depth), BF16), vm((1, depth), F32), vm((4, depth, half), BF16),
            vm((1, half), F32), vm((1, half), F32), vm(queries.shape, BF16), vm(cache_key.shape, BF16),
            vm(cache_value.shape, BF16), pltpu.SMEM((8,), jnp.int32), pltpu.SMEM((8,), jnp.int32),
            vm((rows, depth), BF16), vm((1, 128), F32), vm((1, 128), F32), vm((2, rows, half), jnp.int16),
            vm((2, rows, half), jnp.int16), vm((2, rows, half), F32), vm((2, 1, 128), F32), vm((2, 1, 128), F32), vm((PARTS * 4, 256), BF16),
            vm((2, PARTS, 4, HEAD), BF16), vm((2, PARTS, 4, HEAD), BF16), vm((NZ, 1, 128), F32), vm((16, NZ, 1, 128), F32),
            vm((128, 128), F32),
            dma((16,)), dma((4,)), dma((2,)), dma((2,)), dma((2,)), dma((2,)), dma((2,)), dma((2,)), dma((2,)), dma((2,)), dma((2,)),
            regular, regular,
        ],
        compiler_params=pltpu.CompilerParams(
            collective_id=0, has_side_effects=True, vmem_limit_bytes=66_900_000
        ),
        name="frame_attention",
    )(
        row(token_session), frames, row(ln_gain), w_key, w_value, row(k_bias), row(v_bias), queries, cache_key,
        cache_value, cache_start, cache_len,
    )


def solution(mesh):
    rows = ("grp", "seq")
    return jax.shard_map(
        local,
        mesh=mesh,
        in_specs=(
            P(rows, "mp"), P(rows), P("mp"), P("mp", None), P("mp", None), P("mp"), P("mp"), P(rows, "mp"),
            P(rows, None, "mp"), P(rows, None, "mp"), P(rows), P(rows),
        ),
        out_specs=P(rows, "mp"),
        check_vma=False,
    )
```

```python
import functools

import jax
import jax.numpy as jnp
from jax import lax
from jax.experimental import pallas as pl
from jax.experimental.pallas import tpu as pltpu
from jax.sharding import PartitionSpec as P

HEAD = 128
GROUP = 8
EPSILON = 1e-6
MESH = pl.DeviceIdType.MESH

NZ, NY, NC, NG = 8, 4, 2, 2
PARTS = NG * NZ * NY * NC
F32 = jnp.float32
BF16 = jnp.bfloat16


def kernel(
    tok_hbm, frames_hbm, gain_hbm, wk_hbm, wv_hbm, kb_hbm, vb_hbm, q_hbm, ck_hbm, cv_hbm, start_hbm, len_hbm,
    out_ref,
    tok, frames, gain, weights, kb, vb, q, ck, cv, start, length,
    normed, square_out, square_in, part_out, part_in, own_part, onehot, send, recv, line_tok, all_tok, cached,
    sem_in, sem_w, sem_sq, sem_part_s, sem_part_r, sem_data_s, sem_data_r, sem_line, sem_all, know1, know2,
):
    g, s, m = lax.axis_index("grp"), lax.axis_index("seq"), lax.axis_index("mp")
    core, y, z = lax.rem(s, NC), lax.rem(s // NC, NY), s // (NC * NY)
    me = g * (NZ * NY * NC) + s
    column = (g * NY + y) * NC + core
    rows, depth = frames.shape
    half = kb.shape[1]
    at_g = [g, 1 - g]
    at_z = [z] + [lax.rem(z + d, NZ) * (NY * NC) for d in range(1, NZ)]
    at_z[0] = z * (NY * NC)
    at_y = [y * NC] + [lax.rem(y + d, NY) * NC for d in range(1, NY)]
    at_core = [core, 1 - core]
    at_yc = [[at_y[dy] + at_core[dc] for dc in range(NC)] for dy in range(NY)]

    def turned(dg, dz, dy, dc):
        return (at_g[dg], at_z[dz] + at_yc[dy][dc], m)

    other = (g, s, 1 - m)

    def tell(sem, devices):
        for device in devices:
            pl.semaphore_signal(sem, inc=1, device_id=device, device_id_type=MESH)

    barrier = pltpu.get_barrier_semaphore()
    near = [other] + [turned(0, d, 0, 0) for d in (1, 2, NZ - 2, NZ - 1)]
    near += [turned(0, 0, dy, dc) for dy in range(NY) for dc in range(NC) if dy or dc]
    near += [turned(1, 0, 0, dc) for dc in range(NC)]

    chunk = 32
    loads = [
        pltpu.make_async_copy(
            frames_hbm.at[pl.ds(i * chunk, chunk)], frames.at[pl.ds(i * chunk, chunk)], sem_in.at[i]
        )
        for i in range(rows // chunk)
    ]
    n = len(loads)
    gain_load = pltpu.make_async_copy(gain_hbm, gain, sem_in.at[n])
    tok_load = pltpu.make_async_copy(tok_hbm, tok, sem_in.at[n + 1])
    small = [
        pltpu.make_async_copy(kb_hbm, kb, sem_in.at[n + 2]),
        pltpu.make_async_copy(vb_hbm, vb, sem_in.at[n + 3]),
    ]
    late = [
        pltpu.make_async_copy(q_hbm, q, sem_in.at[n + 4]),
        pltpu.make_async_copy(ck_hbm, ck, sem_in.at[n + 5]),
        pltpu.make_async_copy(cv_hbm, cv, sem_in.at[n + 6]),
        pltpu.make_async_copy(start_hbm, start, sem_in.at[n + 7]),
        pltpu.make_async_copy(len_hbm, length, sem_in.at[n + 8]),
    ]
    for load in loads:
        load.start()
    tell(barrier, near)
    gain_load.start()
    tok_load.start()
    weight_loads = []
    for i, (source, side) in enumerate(((wk_hbm, 1 - m), (wv_hbm, 1 - m), (wk_hbm, m), (wv_hbm, m))):
        load = pltpu.make_async_copy(
            source.at[:, pl.ds(pl.multiple_of(side * half, half), half)], weights.at[i], sem_w.at[i]
        )
        load.start()
        weight_loads.append(load)
    for load in small + late:
        load.start()

    lanes = 128
    square_out[...] = jnp.zeros_like(square_out)
    sums = []
    for i, load in enumerate(loads):
        load.wait()
        total = jnp.zeros((chunk, lanes), F32)
        for j in range(depth // lanes):
            x = frames[pl.ds(i * chunk, chunk), pl.ds(j * lanes, lanes)].astype(F32)
            total = total + x * x
        sums.append(total)
    sums.append(jnp.zeros((lanes - rows, lanes), F32))
    own_squares = jnp.sum(jnp.concatenate(sums, axis=0).T, axis=0, keepdims=True)
    square_out[...] = own_squares
    pl.semaphore_wait(barrier, len(near))
    square_copy = pltpu.make_async_remote_copy(
        square_out, square_in, sem_sq.at[0], sem_sq.at[1], device_id=other, device_id_type=MESH
    )
    square_copy.start()
    tell(know1, [turned(0, 2, 0, 0), turned(0, NZ - 2, 0, 0)] + [turned(0, 0, d, 0) for d in range(1, NY)])

    tok_load.wait()
    padded = jnp.concatenate([tok[...].astype(F32), jnp.full((1, lanes - rows), -8.0 * PARTS, F32)], axis=1)
    line_tok[z] = padded
    row_at = lax.broadcasted_iota(jnp.int32, (1, lanes), 1)
    block = jnp.floor(padded * 0.125)
    block_here = jnp.broadcast_to(block, (lanes, lanes))
    lane_i = lax.broadcasted_iota(jnp.int32, (lanes, lanes), 1)
    sub_i = lax.broadcasted_iota(jnp.int32, (lanes, lanes), 0)
    before = (block_here.T == block_here) & (sub_i < lane_i)
    rank = jnp.sum(before.astype(F32), axis=0, keepdims=True)
    slot = jnp.where(row_at < rows, block * 2.0 + rank, -1.0)
    slot_here = jnp.broadcast_to(slot, (lanes, lanes))
    for p in range(4):
        hit = slot_here == (sub_i // 2 + p * 64).astype(F32)
        for h in range(2):
            onehot[pl.ds(p * lanes, lanes), pl.ds(h * lanes, lanes)] = jnp.where(
                hit & (lax.rem(sub_i, 2) == h), 1.0, 0.0
            ).astype(BF16)

    pl.semaphore_wait(know1, 5)
    group = [
        turned(dg, 0, dy, dc) for dg in range(NG) for dy in range(NY) for dc in range(NC) if dg or dy or dc
    ]
    tell(know2, group)
    for d in range(1, NZ):
        pltpu.make_async_remote_copy(
            line_tok.at[z], line_tok.at[z], sem_line.at[0], sem_line.at[1], device_id=turned(0, d, 0, 0), device_id_type=MESH
        ).start()

    gain_load.wait()
    square_copy.wait()
    squares = square_out[...] + square_in[...]
    inverse = lax.rsqrt(squares / (2 * depth) + EPSILON)
    inverse = jnp.broadcast_to(inverse, (lanes, lanes)).T[:rows]
    step = 512
    first_product = jnp.zeros((rows, half), F32)
    weight_loads[0].wait()
    for j in range(depth // step):
        cols = pl.ds(j * step, step)
        chunk_normed = (frames[:, cols].astype(F32) * inverse[:, :1] * gain[:, cols]).astype(BF16)
        normed[:, cols] = chunk_normed
        first_product = first_product + jnp.dot(chunk_normed, weights[0, cols], preferred_element_type=F32)

    part_copies, top_copies = [], []
    split = part_out.shape[0] // 2
    width = half // split

    def share(product, i):
        for at in range(split):
            piece = product[:, at * width : (at + 1) * width]
            j = i * split + at
            part_out[j] = piece
            copy = pltpu.make_async_remote_copy(
                part_out.at[j], part_in.at[j], sem_part_s.at[j], sem_part_r.at[j], device_id=other, device_id_type=MESH
            )
            copy.start()
            part_copies.append(copy)

    share(first_product, 0)
    for i in range(1, 4):
        weight_loads[i].wait()
        product = jnp.dot(normed[...], weights[i], preferred_element_type=F32)
        if i < 2:
            share(product, i)
        else:
            for at in range(split):
                own_part[(i - 2) * split + at] = product[:, at * width : (at + 1) * width]
    for load in small + late:
        load.wait()

    heads = q.shape[1] // HEAD
    kv_heads = heads // GROUP
    per_shard = q.shape[0]
    stacked = jnp.concatenate([q[:, pl.ds(i * HEAD, HEAD)] for i in range(heads)], axis=0)
    scale = HEAD**-0.5
    window = ck.shape[1]
    slots = lax.broadcasted_iota(jnp.int32, (1, window), 1)
    row_session = lax.broadcasted_iota(jnp.int32, (GROUP * per_shard, lanes), 0)
    row_session = lax.rem(row_session, per_shard)
    for h in range(kv_heads):
        queries = stacked[h * GROUP * per_shard : (h + 1) * GROUP * per_shard]
        score = jnp.zeros((GROUP * per_shard, window), F32)
        for b in range(per_shard):
            keys = ck[b, :, pl.ds(h * HEAD, HEAD)]
            product = lax.dot_general(queries, keys, (((1,), (1,)), ((), ())), preferred_element_type=F32) * scale
            live = lax.rem(slots - start[b] + window, window) < length[b]
            product = jnp.where(live, product, -jnp.inf)
            score = jnp.where(row_session == b, product, score)
        cached[pl.ds(h * GROUP * per_shard, GROUP * per_shard)] = score

    some = pl.ds(0, NZ - 1)
    pltpu.make_async_remote_copy(
        line_tok.at[some], line_tok.at[some], sem_line.at[0], sem_line.at[1], device_id=other, device_id_type=MESH
    ).wait()
    for device in group:
        pltpu.make_async_remote_copy(
            line_tok, all_tok.at[column], sem_all.at[0], sem_all.at[1], device_id=device, device_id_type=MESH
        ).start()
    all_tok[column] = line_tok[...]

    here = column * NZ + z
    peers = [
        (dg, dz, dy, dc)
        for dz in (4, 3, 5, 2, 6, 1, 7, 0) for dg in (1, 0) for dy in (2, 1, 3, 0) for dc in (0, 1)
        if dg or dz or dy or dc
    ]
    peers.sort(key=lambda t: -(2 * t[0] + min(t[1], NZ - t[1]) + min(t[2], NY - t[2])))
    for i in range(2 * split):
        bias = (kb, vb)[i // split][:, (i % split) * width : (i % split + 1) * width]
        part_copies[i].wait()
        whole = (own_part[i] + part_in[i] + bias).astype(BF16)
        parts = []
        for h in range(width // HEAD):
            parts.append(whole[:, h * HEAD : (h + 1) * HEAD])
            parts.append(jnp.zeros((lanes - rows, HEAD), BF16))
        table = jnp.concatenate(parts, axis=0)
        slotted = jnp.dot(onehot[...], table, preferred_element_type=F32).astype(BF16)
        send[i] = slotted.reshape(send.shape[1:])
        if i == 0:
            pl.semaphore_wait(know2, len(group))
        for turn in peers:
            device = turned(*turn)
            to = device[0] * (NZ * NY * NC) + device[1]
            pltpu.make_async_remote_copy(
                send.at[i, to], recv.at[i, here], sem_data_s.at[i], sem_data_r.at[i], device_id=device,
                device_id_type=MESH,
            ).start()
        recv[i, here] = send[i, me]

    some = pl.ds(0, 15)
    pltpu.make_async_remote_copy(
        all_tok.at[some], all_tok.at[some], sem_all.at[0], sem_all.at[1], device_id=other, device_id_type=MESH
    ).wait()
    came = all_tok[...].reshape(PARTS, lanes)
    came_block = jnp.floor(came * 0.125)
    mine = came_block == jnp.full((1, 1), me, jnp.int32).astype(F32)
    upto = jnp.where(sub_i <= lane_i, 1.0, 0.0).astype(BF16)
    rank = jnp.dot(jnp.where(mine, 1.0, 0.0).astype(BF16), upto, preferred_element_type=F32)
    name = jnp.where(mine, came - came_block * 8.0 + 1.0, 0.0)
    first = jnp.sum(jnp.where(rank == 1.0, name, 0.0), axis=1, keepdims=True)
    second = jnp.sum(jnp.where(rank == 2.0, name, 0.0), axis=1, keepdims=True)
    names = jnp.where(lax.rem(lane_i // 2, 2) == 0, first, second)
    names = jnp.where(lane_i // 4 == lax.rem(sub_i, 32), names, 0.0)
    names = [jnp.sum(names[32 * i : 32 * i + 32], axis=0, keepdims=True) for i in range(4)]
    ids_row = jnp.concatenate(names, axis=1)

    def arrived(i):
        everyone = pl.ds(0, PARTS - 1)
        pltpu.make_async_remote_copy(
            send.at[i, everyone], recv.at[i, everyone], sem_data_s.at[i], sem_data_r.at[i], device_id=other,
            device_id_type=MESH,
        ).wait()
        return recv[i].reshape(PARTS * 4, HEAD)

    fresh = lax.dot_general(stacked, arrived(0), (((1,), (1,)), ((), ())), preferred_element_type=F32) * scale
    shape = fresh.shape
    row_i = lax.broadcasted_iota(jnp.int32, shape, 0)
    col_i = lax.broadcasted_iota(jnp.int32, shape, 1)
    match = (ids_row == (lax.rem(row_i, per_shard) + 1).astype(F32)) & (
        lax.rem(col_i, 2) == row_i // (GROUP * per_shard)
    )
    fresh = jnp.where(match, fresh, -jnp.inf)
    held = cached[...]
    largest = jnp.maximum(jnp.max(held, axis=1, keepdims=True), jnp.max(fresh, axis=1, keepdims=True))
    held_exp = jnp.exp(held - largest)
    fresh_exp = jnp.exp(fresh - largest)
    total = jnp.sum(held_exp, axis=1, keepdims=True) + jnp.sum(fresh_exp, axis=1, keepdims=True)
    inverse_total = 1.0 / total
    held_weights = held_exp * inverse_total
    fresh_weights = (fresh_exp * inverse_total).astype(BF16)
    held_terms = []
    for h in range(kv_heads):
        mine = held_weights[h * GROUP * per_shard : (h + 1) * GROUP * per_shard]
        part = jnp.zeros((GROUP * per_shard, HEAD), F32)
        for b in range(per_shard):
            only = jnp.where(row_session == b, mine, 0.0).astype(BF16)
            part = part + jnp.dot(only, cv[b, :, pl.ds(h * HEAD, HEAD)], preferred_element_type=F32)
        held_terms.append(part)
    held_terms = jnp.concatenate(held_terms, axis=0)

    result = held_terms + jnp.dot(fresh_weights, arrived(1), preferred_element_type=F32)
    for i in range(heads):
        out_ref[:, pl.ds(i * HEAD, HEAD)] = result[i * per_shard : (i + 1) * per_shard].astype(BF16)


def local(
    frames, token_session, ln_gain, w_key, w_value, k_bias, v_bias, queries, cache_key, cache_value, cache_start,
    cache_len,
):
    rows, depth = frames.shape
    half = k_bias.shape[0]
    row = lambda a: a.reshape(1, -1)
    anywhere = pl.BlockSpec(memory_space=pltpu.HBM)
    dma = pltpu.SemaphoreType.DMA
    regular = pltpu.SemaphoreType.REGULAR
    vm = pltpu.VMEM
    return pl.pallas_call(
        kernel,
        out_shape=pltpu.VMEM(queries.shape, BF16),
        in_specs=[anywhere] * 12,
        out_specs=pl.BlockSpec(memory_space=pltpu.VMEM),
        scratch_shapes=[
            vm((1, rows), jnp.int32), vm((rows, depth), BF16), vm((1, depth), F32), vm((4, depth, half), BF16),
            vm((1, half), F32), vm((1, half), F32), vm(queries.shape, BF16), vm(cache_key.shape, BF16),
            vm(cache_value.shape, BF16), pltpu.SMEM((8,), jnp.int32), pltpu.SMEM((8,), jnp.int32),
            vm((rows, depth), BF16), vm((1, 128), F32), vm((1, 128), F32), vm((2, rows, half), F32),
            vm((2, rows, half), F32), vm((2, rows, half), F32), vm((PARTS * 4, 256), BF16),
            vm((2, PARTS, 4, HEAD), BF16), vm((2, PARTS, 4, HEAD), BF16), vm((NZ, 1, 128), F32), vm((16, NZ, 1, 128), F32),
            vm((128, 128), F32),
            dma((16,)), dma((4,)), dma((2,)), dma((2,)), dma((2,)), dma((2,)), dma((2,)), dma((2,)), dma((2,)),
            regular, regular,
        ],
        compiler_params=pltpu.CompilerParams(
            collective_id=0, has_side_effects=True, vmem_limit_bytes=66_900_000
        ),
        name="frame_attention",
    )(
        row(token_session), frames, row(ln_gain), w_key, w_value, row(k_bias), row(v_bias), queries, cache_key,
        cache_value, cache_start, cache_len,
    )


def solution(mesh):
    rows = ("grp", "seq")
    return jax.shard_map(
        local,
        mesh=mesh,
        in_specs=(
            P(rows, "mp"), P(rows), P("mp"), P("mp", None), P("mp", None), P("mp"), P("mp"), P(rows, "mp"),
            P(rows, None, "mp"), P(rows, None, "mp"), P(rows), P(rows),
        ),
        out_specs=P(rows, "mp"),
        check_vma=False,
    )
```
